512 devices in a mesh: gx: 16 (over y_hi, z), gy: 4 (over y_lo), gz: 8 (over x, core).
Axes of the slice: x: 4, y: 8 (y_hi: 2, y_lo: 4; y = y_hi * 4 + y_lo), z: 8, core: 2. Of those that a mesh axis runs over, the one named last changes fastest.
Arguments:
- pair: bfloat16 [512, 512, 128], P('gx', ('gy', 'gz')), may hold values from -6 to 6
- pair_mask: int32 [512, 512], P('gx', ('gy', 'gz')), may hold values 0 or 1
- in_gain: float32 [128], replicated, may hold values from 0.1 to 1.9
- in_bias: float32 [128], replicated, may hold values from -3 to 3
- proj_weight: bfloat16 [128, 512], replicated, may hold values from -0.5 to 0.5
- gate_weight: bfloat16 [128, 128], replicated, may hold values from -0.5 to 0.5
- out_gain: float32 [128], replicated, may hold values from 0.1 to 1.9
- out_bias: float32 [128], replicated, may hold values from -3 to 3
- out_weight: bfloat16 [128, 128], replicated, may hold values from -0.5 to 0.5
Outputs:
- update: bfloat16 [512, 512, 128], P('gx', ('gy', 'gz'))
The draws below stay inside these ranges and needn't reach their ends.
All inputs are finite; a program needn't handle non-finite values. No bound on the sum of `pair_mask` on one device may be relied on, other than what follows from the above.
Results may differ from the reference program's by a relative error of at most 0.0071.
Values may be sent and summed in bfloat16 or wider, within the bound.
No kernel may reach another device: no remote copies, remote signals or barrier semaphores. Data moves between devices by JAX's collectives and lax.ppermute only.
A program may use at most 64 MiB of HBM per device.

```python
import jax
import jax.numpy as jnp
from jax import lax

C = 128
CH = 128
N = 512


def with_ends(array, stream_key, smallest, high):
    spot = [jax.random.randint(jax.random.fold_in(stream_key, axis), (), 0, length) for axis, length in enumerate(array.shape)]
    widest = array.shape.index(max(array.shape))
    beside = spot[:widest] + [(spot[widest] + 1) % array.shape[widest]] + spot[widest + 1:]
    return array.at[tuple(spot)].set(smallest).at[tuple(beside)].set(high)


def block_levels(stream_key, shape, pieces, low, largest):
    loudness = 1.0
    for axis_at, parts in pieces:
        steps = jax.random.uniform(jax.random.fold_in(jax.random.fold_in(stream_key, 6), axis_at), (parts,), jnp.float32, low / len(pieces), largest / len(pieces))
        loudness = loudness * jnp.repeat(jnp.exp(steps), shape[axis_at] // parts).reshape((-1,) + (1,) * (len(shape) - 1 - axis_at))
    return loudness


def gaussian(key, shape, scale, reach, split=(), held_as=jnp.bfloat16):
    result = scale * jax.random.normal(key, shape, jnp.float32)
    if split:
        result = result * block_levels(key, shape, split, -0.22, 0.18)
    return jnp.clip(result, -reach, reach).astype(held_as)


def setup_inputs(seed: int = 0) -> dict:
    splits = jax.random.split(jax.random.key(seed), 10)
    pair = gaussian(splits[0], (N, N, C), 1.0, 6.0, ((0, 16), (1, 32)))
    pair_mask = with_ends((jax.random.randint(splits[1], (N, N), 0, 4) < 3).astype(jnp.int32), jax.random.fold_in(splits[1], 1), 0, 1)
    in_gain = jnp.clip(1.0 + 0.18 * jax.random.normal(splits[2], (C,), jnp.float32), 0.1, 1.9)
    in_bias = gaussian(splits[3], (C,), 0.5, 3.0, (), jnp.float32)
    proj_weight = gaussian(splits[4], (C, 4 * CH), C ** -0.5, 0.5)
    gate_weight = gaussian(splits[5], (C, C), C ** -0.5, 0.5)
    out_gain = jnp.clip(1.0 + 0.18 * jax.random.normal(splits[6], (CH,), jnp.float32), 0.1, 1.9)
    out_bias = gaussian(splits[7], (CH,), 0.5, 3.0, (), jnp.float32)
    out_weight = gaussian(splits[8], (CH, C), CH ** -0.5, 0.5)
    return dict(pair=pair, pair_mask=pair_mask, in_gain=in_gain, in_bias=in_bias, proj_weight=proj_weight, gate_weight=gate_weight, out_gain=out_gain, out_bias=out_bias, out_weight=out_weight)


def normalize(values, gain, bias):
    average = lax.optimization_barrier(jnp.mean(values, axis=-1, keepdims=True))
    centered = values - average
    variance = lax.optimization_barrier(jnp.mean(centered * centered, axis=-1, keepdims=True))
    return centered * lax.rsqrt(variance + 1e-05) * gain + bias

def reference(pair, pair_mask, in_gain, in_bias, proj_weight, gate_weight, out_gain, out_bias, out_weight):
    total = pair.shape[0]
    channels = pair.shape[2]
    hidden = proj_weight.shape[1] // 4
    normed = normalize(pair.astype(jnp.float32), in_gain, in_bias).astype(jnp.bfloat16)
    flat = normed.reshape(total * total, channels)
    projected = jnp.dot(flat, proj_weight, preferred_element_type=jnp.float32).reshape(total, total, 4 * hidden)
    mask_value = pair_mask.astype(jnp.float32)[:, :, None]
    left_side = (jax.nn.sigmoid(projected[:, :, :hidden]) * projected[:, :, hidden:2 * hidden] * mask_value).astype(jnp.bfloat16)
    right_side = (jax.nn.sigmoid(projected[:, :, 2 * hidden:3 * hidden]) * projected[:, :, 3 * hidden:] * mask_value).astype(jnp.bfloat16)
    triangle = jnp.einsum('ikc,jkc->ijc', left_side.astype(jnp.float32), right_side.astype(jnp.float32), precision=lax.Precision.HIGHEST)
    tri_normed = normalize(triangle, out_gain, out_bias).astype(jnp.bfloat16)
    gating = jax.nn.sigmoid(jnp.dot(flat, gate_weight, preferred_element_type=jnp.float32))
    mixed = jnp.dot(tri_normed.reshape(total * total, hidden), out_weight, preferred_element_type=jnp.float32)
    return (gating * mixed).reshape(total, total, channels).astype(jnp.bfloat16)
```

```python
import functools

import jax
import jax.numpy as jnp
from jax import lax
from jax.experimental import pallas as pl
from jax.experimental.pallas import tpu as pltpu
from jax.sharding import Mesh
from jax.sharding import PartitionSpec as P

COLUMNS = ("co", "gy", "x")
OUT_ORDER = ("gx", *COLUMNS)
IN_ORDER = (*COLUMNS, "gx")
EPS = 1e-05
F32 = jnp.float32
BF16 = jnp.bfloat16


def lane_iota(shape):
    return lax.broadcasted_iota(jnp.int32, shape, len(shape) - 1)


def swap_bits(arrays, bits):
    arrays = list(arrays)
    lanes = lane_iota(arrays[0].shape)
    for pos, lane in bits:
        step, width = 1 << pos, 1 << lane
        high = (lanes & width) != 0
        for at in range(len(arrays)):
            if at & step:
                continue
            a, b = arrays[at], arrays[at + step]
            arrays[at] = jnp.where(high, pltpu.roll(b, width, 1), a)
            arrays[at + step] = jnp.where(high, b, pltpu.roll(a, 128 - width, 1))
    return arrays


def project_kernel(pair, mask, gain, bias, weight, sent, normed_out, rows):
    x = pair[...].astype(F32)
    centered = x - jnp.mean(x, axis=-1, keepdims=True)
    variance = jnp.mean(centered * centered, axis=-1, keepdims=True)
    normed = (centered * lax.rsqrt(variance + EPS) * gain[...] + bias[...]).astype(BF16)
    normed_out[...] = normed
    k_of_lane = lane_iota((16, 128)) & 15
    spread = (k_of_lane == lax.broadcasted_iota(jnp.int32, (16, 128), 0)).astype(BF16)
    masks = jnp.dot(mask[...].astype(F32).astype(BF16), spread, preferred_element_type=F32)
    own_row = (lane_iota((8, 128)) >> 4) == lax.broadcasted_iota(jnp.int32, (8, 128), 0)
    for q in range(4):
        projected = lax.dot_general(
            weight[...],
            normed[q * 128 : (q + 1) * 128],
            (((0,), (1,)), ((), ())),
            preferred_element_type=F32,
        )
        keep = jnp.sum(jnp.where(own_row, masks[q * 8 : (q + 1) * 8], 0.0), axis=0, keepdims=True)
        left = jax.nn.sigmoid(projected[:128]) * projected[128:256] * keep
        right = jax.nn.sigmoid(projected[256:384]) * projected[384:] * keep
        hi, lo = q // 2, q % 2
        for other in range(2):
            for c_hi in range(4):
                block = slice(c_hi * 32, (c_hi + 1) * 32)
                to_left = ((hi * 2 + other) * 4 + c_hi) * 4 + lo
                rows[pl.ds(to_left, 32, stride=64), :] = left[block]
                to_right = ((other * 2 + lo) * 4 + c_hi) * 4 + 2 + hi
                rows[pl.ds(to_right, 32, stride=64), :] = right[block]
    sent[...] = rows[...].astype(BF16)


def triangle_kernel(got, sent, rows, left, right, product):
    rows[...] = got[...].astype(F32)
    for slot in range(4):
        for g_hi in range(4):
            pieces = [
                rows[pl.ds((g_hi * 8 + g) * 64 + slot, 16, stride=4), :] for g in range(8)
            ]
            pieces = swap_bits(pieces, ((0, 4), (1, 5), (2, 6)))
            for r in range(8):
                piece = pieces[r].astype(BF16)
                lanes = pl.ds(g_hi * 128, 128)
                if slot < 2:
                    left[pl.ds(((r % 2 * 2 + slot) * 4 + r // 2) * 16, 16), lanes] = piece
                else:
                    right[pl.ds((r * 2 + slot - 2) * 16, 16), lanes] = piece
    product[...] = lax.dot_general(
        right[...], left[...], (((1,), (1,)), ((), ())), preferred_element_type=F32
    )
    for at in range(4):
        pieces = [
            product[pl.ds(v % 8 * 32 + at * 8, 8), pl.ds(v // 8 * 128, 128)] for v in range(16)
        ]
        pieces = swap_bits(pieces, ((0, 0), (1, 1), (2, 2), (3, 3)))
        for gx in range(16):
            sent[pl.ds(gx * 32 + at * 8, 8), :] = pieces[gx]


def mix_kernel(got, normed, gate_weight, gain, bias, out_weight, update):
    gating = jax.nn.sigmoid(jnp.dot(normed[...], gate_weight[...], preferred_element_type=F32))
    gains = jnp.broadcast_to(gain[...], (128, 128)).T
    biases = jnp.broadcast_to(bias[...], (128, 128)).T
    for ih in range(2):
        halves = []
        gates = gating[ih * 256 : (ih + 1) * 256].reshape(16, 2, 8, 128)
        for jh in range(2):
            triangle = got[pl.ds((ih * 2 + jh) * 128, 128), :]
            centered = triangle - jnp.mean(triangle, axis=0, keepdims=True)
            variance = jnp.mean(centered * centered, axis=0, keepdims=True)
            tri_normed = (centered * lax.rsqrt(variance + EPS) * gains + biases).astype(BF16)
            mixed = lax.dot_general(
                tri_normed, out_weight[...], (((0,), (0,)), ((), ())), preferred_element_type=F32
            )
            halves.append(mixed.reshape(16, 8, 128) * gates[:, jh])
        both = jnp.concatenate(halves, axis=1).reshape(256, 128)
        update[pl.ds(ih * 256, 256), :] = both.astype(BF16)


def local_call(kernel, outs, scratch=(), flops=1_000_000):
    vmem = pl.BlockSpec(memory_space=pltpu.VMEM)

    def call(*args):
        return pl.pallas_call(
            kernel,
            out_shape=outs,
            in_specs=[vmem] * len(args),
            out_specs=jax.tree.map(lambda _: vmem, outs),
            scratch_shapes=scratch,
            compiler_params=pltpu.CompilerParams(vmem_limit_bytes=16 << 20),
            cost_estimate=pl.CostEstimate(
                flops=flops, bytes_accessed=1 << 20, transcendentals=0
            ),
        )(*args)

    return call


def on_device(
    pair, pair_mask, in_gain, in_bias, proj_weight, gate_weight, out_gain, out_bias, out_weight
):
    shape = jax.ShapeDtypeStruct
    sent, normed = local_call(
        project_kernel,
        (shape((2048, 128), BF16), shape((512, 128), BF16)),
        [pltpu.VMEM((2048, 128), F32)],
    )(pair.reshape(512, 128), pair_mask, in_gain[None], in_bias[None], proj_weight)
    got = lax.all_to_all(sent.reshape(512, 4, 128), IN_ORDER, 0, 0, tiled=True)
    sums = local_call(
        triangle_kernel,
        shape((512, 128), F32),
        [
            pltpu.VMEM((2048, 128), F32),
            pltpu.VMEM((256, 512), BF16),
            pltpu.VMEM((256, 512), BF16),
            pltpu.VMEM((256, 256), F32),
        ],
    )(got.reshape(2048, 128))
    back = lax.all_to_all(sums.reshape(512, 1, 128), OUT_ORDER, 0, 0, tiled=True)
    update = local_call(mix_kernel, shape((512, 128), BF16))(
        back.reshape(512, 128), normed, gate_weight, out_gain[None], out_bias[None], out_weight
    )
    return update.reshape(32, 16, 128)


def solution(mesh):
    gx, gy, gz = (mesh.shape[name] for name in ("gx", "gy", "gz"))
    finer = Mesh(mesh.devices.reshape(gx, gy, gz // 2, 2), ("gx", "gy", "x", "co"))
    columns = ("gy", "x", "co")
    in_specs = (P("gx", columns, None), P("gx", columns), P(), P(), P(), P(), P(), P(), P())
    return jax.shard_map(
        on_device,
        mesh=finer,
        in_specs=in_specs,
        out_specs=P("gx", columns, None),
        check_vma=False,
    )
```

```python
import jax
import jax.numpy as jnp
from jax import lax
from jax.experimental import pallas as pl
from jax.experimental.pallas import tpu as pltpu
from jax.sharding import Mesh
from jax.sharding import PartitionSpec as P

ROW_AXES = ("yh", "zh", "zl")
COLUMN_AXES = ("y1", "y0", "x1", "x0", "co")
IN_ORDER = (*COLUMN_AXES, "yh", "zl")
OUT_ORDER = ("zl", "yh", *COLUMN_AXES)
EPS = 1e-05
F32 = jnp.float32
BF16 = jnp.bfloat16


def lane_iota(shape):
    return lax.broadcasted_iota(jnp.int32, shape, len(shape) - 1)


def swap_bits(arrays, bits):
    arrays = list(arrays)
    lanes = lane_iota(arrays[0].shape)
    for pos, lane in bits:
        step, width = 1 << pos, 1 << lane
        high = (lanes & width) != 0
        for at in range(len(arrays)):
            if at & step:
                continue
            a, b = arrays[at], arrays[at + step]
            arrays[at] = jnp.where(high, pltpu.roll(b, width, 1), a)
            arrays[at + step] = jnp.where(high, b, pltpu.roll(a, 128 - width, 1))
    return arrays


def project_kernel(
    pair_hbm,
    mask_hbm,
    gain_hbm,
    bias_hbm,
    weight_hbm,
    out_gain_hbm,
    out_bias_hbm,
    sent,
    normed_out,
    scales,
    pair,
    mask,
    gain,
    bias,
    weight,
    rows,
    sems,
):
    copies = [
        pltpu.make_async_copy(source, target, sems.at[at])
        for at, (source, target) in enumerate(
            (
                (pair_hbm, pair),
                (weight_hbm, weight),
                (mask_hbm, mask),
                (gain_hbm, gain),
                (bias_hbm, bias),
                (out_gain_hbm, scales.at[pl.ds(0, 1)]),
                (out_bias_hbm, scales.at[pl.ds(1, 1)]),
            )
        )
    ]
    for copy in copies:
        copy.start()
    for copy in copies:
        copy.wait()
    x = pair[...].astype(F32)
    centered = x - jnp.mean(x, axis=-1, keepdims=True)
    variance = jnp.mean(centered * centered, axis=-1, keepdims=True)
    normed = (centered * lax.rsqrt(variance + EPS) * gain[...] + bias[...]).astype(BF16)
    normed_out[...] = normed
    k_of_lane = lane_iota((16, 128)) & 15
    spread = (k_of_lane == lax.broadcasted_iota(jnp.int32, (16, 128), 0)).astype(BF16)
    masks = lax.dot_general(
        mask[...].astype(F32).astype(BF16),
        spread,
        (((0,), (0,)), ((), ())),
        preferred_element_type=F32,
    )
    own_row = (lane_iota((8, 128)) >> 4) == lax.broadcasted_iota(jnp.int32, (8, 128), 0)
    for q in range(4):
        projected = lax.dot_general(
            weight[...],
            normed[q * 128 : (q + 1) * 128],
            (((0,), (1,)), ((), ())),
            preferred_element_type=F32,
        )
        keep = jnp.sum(jnp.where(own_row, masks[q * 8 : (q + 1) * 8], 0.0), axis=0, keepdims=True)
        left = jax.nn.sigmoid(projected[:128]) * projected[128:256] * keep
        right = jax.nn.sigmoid(projected[256:384]) * projected[384:] * keep
        for c_hi in range(4):
            block = slice(c_hi * 32, (c_hi + 1) * 32)
            at = (c_hi % 2 * 2 + c_hi // 2) * 8 + q * 2
            rows[pl.ds(at, 32, stride=32), :] = left[block]
            rows[pl.ds(at + 1, 32, stride=32), :] = right[block]
    sent[...] = rows[...].astype(BF16)


def sides_kernel(got, left, right, rows):
    rows[...] = got[...].astype(F32)
    for side, target in enumerate((left, right)):
        for g_hi in range(4):
            pieces = [
                rows[pl.ds((g_hi * 8 + g) * 32 + side, 16, stride=2), :] for g in range(8)
            ]
            pieces = swap_bits(pieces, ((0, 4), (1, 5), (2, 6)))
            for r in range(8):
                target[pl.ds(r * 16, 16), pl.ds(g_hi * 128, 128)] = pieces[r].astype(BF16)


def triangle_kernel(right, left, sent, product, rows):
    product[...] = lax.dot_general(
        right[...], left[...], (((1,), (1,)), ((), ())), preferred_element_type=F32
    )
    for zh in range(4):
        for yh_j in range(2):
            pieces = [product[pl.ds(zh * 128 + r * 16 + yh_j * 8, 8), :] for r in range(8)]
            pieces = swap_bits(pieces, ((0, 2), (1, 3)))
            for v in range(8):
                high, yh, zl = v >> 2, v >> 1 & 1, v & 1
                owner = zl * 64 + yh * 32 + yh_j * 16 + zh * 4
                rows[pl.ds(owner * 4 + high, 8, stride=2), :] = pieces[v]
    sent[...] = rows[...].astype(BF16)


def mix_kernel(got, normed, gate_weight, scales, out_weight, update, rows, mixed, ordered):
    rows[...] = got[...].astype(F32)
    gating = jax.nn.sigmoid(jnp.dot(normed[...], gate_weight[...], preferred_element_type=F32))
    gains = jnp.broadcast_to(scales[0:1, :], (128, 128)).T
    biases = jnp.broadcast_to(scales[1:2, :], (128, 128)).T
    for h in range(4):
        triangle = rows[pl.ds(h, 128, stride=4), :]
        centered = triangle - jnp.mean(triangle, axis=0, keepdims=True)
        variance = jnp.mean(centered * centered, axis=0, keepdims=True)
        tri_normed = (centered * lax.rsqrt(variance + EPS) * gains + biases).astype(BF16)
        mixed[pl.ds(h * 128, 128), :] = lax.dot_general(
            tri_normed, out_weight[...], (((0,), (0,)), ((), ())), preferred_element_type=F32
        )
        for s in range(4):
            for jj in range(4):
                ordered[pl.ds(s * 128 + h * 4 + jj, 8, stride=16), :] = mixed[
                    pl.ds(h * 128 + jj * 4 + s, 8, stride=16), :
                ]
    update[...] = (ordered[...] * gating).astype(BF16)


def local_call(kernel, outs, scratch=(), flops=1_000_000, space=pltpu.VMEM):
    vmem = pl.BlockSpec(memory_space=pltpu.VMEM)

    def call(*args):
        return pl.pallas_call(
            kernel,
            out_shape=outs,
            in_specs=[pl.BlockSpec(memory_space=space)] * len(args),
            out_specs=jax.tree.map(lambda _: vmem, outs),
            scratch_shapes=scratch,
            compiler_params=pltpu.CompilerParams(vmem_limit_bytes=16 << 20),
            cost_estimate=pl.CostEstimate(
                flops=flops, bytes_accessed=1 << 20, transcendentals=0
            ),
        )(*args)

    return call


def on_device(
    pair, pair_mask, in_gain, in_bias, proj_weight, gate_weight, out_gain, out_bias, out_weight
):
    shape = jax.ShapeDtypeStruct
    sent, normed, scales = local_call(
        project_kernel,
        (shape((1024, 128), BF16), shape((512, 128), BF16), shape((2, 128), F32)),
        [
            pltpu.VMEM((512, 128), BF16),
            pltpu.VMEM((16, 32), jnp.int32),
            pltpu.VMEM((1, 128), F32),
            pltpu.VMEM((1, 128), F32),
            pltpu.VMEM((128, 512), BF16),
            pltpu.VMEM((1024, 128), F32),
            pltpu.SemaphoreType.DMA((7,)),
        ],
        space=pltpu.HBM,
    )(
        pair.reshape(512, 128),
        pair_mask.T,
        in_gain[None],
        in_bias[None],
        proj_weight,
        out_gain[None],
        out_bias[None],
    )
    got = lax.all_to_all(sent.reshape(128, 8, 128), IN_ORDER, 0, 0, tiled=True)
    left, right = local_call(
        sides_kernel,
        (shape((128, 512), BF16), shape((128, 512), BF16)),
        [pltpu.VMEM((1024, 128), F32)],
    )(got.reshape(1024, 128))
    every_right = lax.all_gather(right, "zh", axis=0, tiled=True)
    sums = local_call(
        triangle_kernel,
        shape((512, 128), BF16),
        [pltpu.VMEM((512, 128), F32), pltpu.VMEM((512, 128), F32)],
    )(every_right, left)
    back = lax.all_to_all(sums.reshape(128, 4, 128), OUT_ORDER, 0, 0, tiled=True)
    update = local_call(
        mix_kernel,
        shape((512, 128), BF16),
        [pltpu.VMEM((512, 128), F32), pltpu.VMEM((512, 128), F32), pltpu.VMEM((512, 128), F32)],
    )(back.reshape(512, 128), normed, gate_weight, scales, out_weight)
    return update.reshape(32, 16, 128)


def solution(mesh):
    finer = Mesh(mesh.devices.reshape((2, 4) + (2,) * 6), ROW_AXES + COLUMN_AXES)
    in_specs = (
        P(ROW_AXES, COLUMN_AXES, None),
        P(ROW_AXES, COLUMN_AXES),
        P(),
        P(),
        P(),
        P(),
        P(),
        P(),
        P(),
    )
    return jax.shard_map(
        on_device,
        mesh=finer,
        in_specs=in_specs,
        out_specs=P(ROW_AXES, COLUMN_AXES, None),
        check_vma=False,
    )
```

```python
import jax
import jax.numpy as jnp
from jax import lax
from jax.experimental import pallas as pl
from jax.experimental.pallas import tpu as pltpu
from jax.sharding import Mesh
from jax.sharding import PartitionSpec as P

ROW_AXES = ("yh", "zh", "zl")
COLUMN_AXES = ("y1", "y0", "x1", "x0", "co")
ORDER = (*COLUMN_AXES, "yh", "zl")
EPS = 1e-05
F32 = jnp.float32
BF16 = jnp.bfloat16


def lane_iota(shape):
    return lax.broadcasted_iota(jnp.int32, shape, len(shape) - 1)


def swap_bits(arrays, bits):
    arrays = list(arrays)
    lanes = lane_iota(arrays[0].shape)
    for pos, lane in bits:
        step, width = 1 << pos, 1 << lane
        high = (lanes & width) != 0
        for at in range(len(arrays)):
            if at & step:
                continue
            a, b = arrays[at], arrays[at + step]
            arrays[at] = jnp.where(high, pltpu.roll(b, width, 1), a)
            arrays[at + step] = jnp.where(high, b, pltpu.roll(a, 128 - width, 1))
    return arrays


def normalize_kernel(pair, normalized):
    x = pair[...].astype(F32)
    centered = x - jnp.mean(x, axis=-1, keepdims=True)
    variance = jnp.mean(centered * centered, axis=-1, keepdims=True)
    normalized[...] = centered * lax.rsqrt(variance + EPS)


def project_kernel(
    normalized, mask, gain, bias, weight, out_gain, out_bias, sent, normed_out, scales, rows
):
    scales[0:1, :] = out_gain[...]
    scales[1:2, :] = out_bias[...]
    normed = (normalized[...] * gain[...] + bias[...]).astype(BF16)
    normed_out[...] = normed
    k_of_lane = lane_iota((16, 128)) & 15
    spread = (k_of_lane == lax.broadcasted_iota(jnp.int32, (16, 128), 0)).astype(BF16)
    masks = lax.dot_general(
        mask[...].astype(F32).astype(BF16),
        spread,
        (((0,), (0,)), ((), ())),
        preferred_element_type=F32,
    )
    own_row = (lane_iota((8, 128)) >> 4) == lax.broadcasted_iota(jnp.int32, (8, 128), 0)
    for q in range(4):
        projected = lax.dot_general(
            weight[...],
            normed[q * 128 : (q + 1) * 128],
            (((0,), (1,)), ((), ())),
            preferred_element_type=F32,
        )
        keep = jnp.sum(jnp.where(own_row, masks[q * 8 : (q + 1) * 8], 0.0), axis=0, keepdims=True)
        rows[pl.ds(q * 2, 128, stride=8), :] = (
            jax.nn.sigmoid(projected[:128]) * projected[128:256] * keep
        )
        rows[pl.ds(q * 2 + 1, 128, stride=8), :] = (
            jax.nn.sigmoid(projected[256:384]) * projected[384:] * keep
        )
    sent[...] = rows[...].astype(BF16)


def sides_kernel(got, left, right, rows):
    rows[...] = got[...].astype(F32)
    for side, target in enumerate((left, right)):
        for g_hi in range(4):
            pieces = [
                rows[pl.ds((g_hi * 8 + g) * 32 + side, 16, stride=2), :] for g in range(8)
            ]
            pieces = swap_bits(pieces, ((0, 4), (1, 5), (2, 6)))
            for r in range(8):
                target[pl.ds(r * 16, 16), pl.ds(g_hi * 128, 128)] = pieces[r].astype(BF16)


def triangle_kernel(right, left, sent, product, rows):
    product[...] = lax.dot_general(
        right[...], left[...], (((1,), (1,)), ((), ())), preferred_element_type=F32
    )
    for zh in range(4):
        for jh in range(2):
            pieces = [product[pl.ds(zh * 128 + r * 16 + jh, 8, stride=2), :] for r in range(8)]
            pieces = swap_bits(pieces, ((0, 2), (1, 3)))
            for v in range(8):
                high, owner_row = v >> 2, v & 3
                for yh in range(2):
                    at = ((yh * 16 + zh * 4) * 4 + owner_row) * 4 + jh * 2 + high
                    rows[pl.ds(at, 4, stride=16), :] = pieces[v][yh * 4 : yh * 4 + 4]
    sent[...] = rows[...].astype(BF16)


def mix_kernel(got, normed, gate_weight, scales, out_weight, update, rows, mixed, ordered):
    rows[...] = got[...].astype(F32)
    gating = jax.nn.sigmoid(jnp.dot(normed[...], gate_weight[...], preferred_element_type=F32))
    gains = jnp.broadcast_to(scales[0:1, :], (128, 128)).T
    biases = jnp.broadcast_to(scales[1:2, :], (128, 128)).T
    for h in range(4):
        triangle = rows[pl.ds(h, 128, stride=4), :]
        centered = triangle - jnp.mean(triangle, axis=0, keepdims=True)
        variance = jnp.mean(centered * centered, axis=0, keepdims=True)
        tri_normed = (centered * lax.rsqrt(variance + EPS) * gains + biases).astype(BF16)
        mixed[pl.ds(h * 128, 128), :] = lax.dot_general(
            tri_normed, out_weight[...], (((0,), (0,)), ((), ())), preferred_element_type=F32
        )
        for s in range(4):
            for jj in range(4):
                ordered[pl.ds(s * 128 + h * 4 + jj, 8, stride=16), :] = mixed[
                    pl.ds(h * 128 + jj * 4 + s, 8, stride=16), :
                ]
    update[...] = (ordered[...] * gating).astype(BF16)


def local_call(kernel, outs, scratch=(), flops=1_000_000):
    vmem = pl.BlockSpec(memory_space=pltpu.VMEM)

    def call(*args):
        return pl.pallas_call(
            kernel,
            out_shape=outs,
            in_specs=[vmem] * len(args),
            out_specs=jax.tree.map(lambda _: vmem, outs),
            scratch_shapes=scratch,
            compiler_params=pltpu.CompilerParams(vmem_limit_bytes=16 << 20),
            cost_estimate=pl.CostEstimate(
                flops=flops, bytes_accessed=1 << 20, transcendentals=0
            ),
        )(*args)

    return call


def on_device(
    pair, pair_mask, in_gain, in_bias, proj_weight, gate_weight, out_gain, out_bias, out_weight
):
    shape = jax.ShapeDtypeStruct
    normalized = local_call(normalize_kernel, shape((512, 128), F32))(pair.reshape(512, 128))
    sent, normed, scales = local_call(
        project_kernel,
        (shape((1024, 128), BF16), shape((512, 128), BF16), shape((2, 128), F32)),
        [pltpu.VMEM((1024, 128), F32)],
    )(
        normalized,
        pair_mask.T,
        in_gain[None],
        in_bias[None],
        proj_weight,
        out_gain[None],
        out_bias[None],
    )
    got = lax.all_to_all(sent.reshape(128, 8, 128), ORDER, 0, 0, tiled=True)
    left, right = local_call(
        sides_kernel,
        (shape((128, 512), BF16), shape((128, 512), BF16)),
        [pltpu.VMEM((1024, 128), F32)],
    )(got.reshape(1024, 128))
    every_right = lax.all_gather(right, "zh", axis=0, tiled=True)
    sums = local_call(
        triangle_kernel,
        shape((512, 128), BF16),
        [pltpu.VMEM((512, 128), F32), pltpu.VMEM((512, 128), F32)],
    )(every_right, left)
    back = lax.all_to_all(sums.reshape(128, 4, 128), ORDER, 0, 0, tiled=True)
    update = local_call(
        mix_kernel,
        shape((512, 128), BF16),
        [pltpu.VMEM((512, 128), F32), pltpu.VMEM((512, 128), F32), pltpu.VMEM((512, 128), F32)],
    )(back.reshape(512, 128), normed, gate_weight, scales, out_weight)
    return update.reshape(32, 16, 128)


def solution(mesh):
    finer = Mesh(mesh.devices.reshape((2, 4) + (2,) * 6), ROW_AXES + COLUMN_AXES)
    in_specs = (
        P(ROW_AXES, COLUMN_AXES, None),
        P(ROW_AXES, COLUMN_AXES),
        P(),
        P(),
        P(),
        P(),
        P(),
        P(),
        P(),
    )
    return jax.shard_map(
        on_device,
        mesh=finer,
        in_specs=in_specs,
        out_specs=P(ROW_AXES, COLUMN_AXES, None),
        check_vma=False,
    )
```

```python
import jax
import jax.numpy as jnp
from jax import lax
from jax.experimental import pallas as pl
from jax.experimental.pallas import tpu as pltpu
from jax.sharding import Mesh
from jax.sharding import PartitionSpec as P

ROW_AXES = ("yh", "zh", "zl")
COLUMN_AXES = ("y1", "y0", "x1", "x0", "co")
ORDER = (*COLUMN_AXES, "yh", "zl")
EPS = 1e-05
F32 = jnp.float32
BF16 = jnp.bfloat16


def lane_iota(shape):
    return lax.broadcasted_iota(jnp.int32, shape, len(shape) - 1)


def swap_bits(arrays, bits):
    arrays = list(arrays)
    lanes = lane_iota(arrays[0].shape)
    for pos, lane in bits:
        step, width = 1 << pos, 1 << lane
        high = (lanes & width) != 0
        for at in range(len(arrays)):
            if at & step:
                continue
            a, b = arrays[at], arrays[at + step]
            arrays[at] = jnp.where(high, pltpu.roll(b, width, 1), a)
            arrays[at + step] = jnp.where(high, b, pltpu.roll(a, 128 - width, 1))
    return arrays


def project_kernel(
    pair_hbm,
    weight_hbm,
    mask_hbm,
    gain_hbm,
    bias_hbm,
    out_gain_hbm,
    out_bias_hbm,
    sent,
    normed_out,
    scales,
    pair,
    weight,
    mask,
    gain,
    bias,
    rows,
    sems,
):
    moves = (
        (pair_hbm, pair),
        (gain_hbm, gain),
        (bias_hbm, bias),
        (weight_hbm, weight),
        (mask_hbm, mask),
        (out_gain_hbm, scales.at[pl.ds(0, 1)]),
        (out_bias_hbm, scales.at[pl.ds(1, 1)]),
    )
    copies = [
        pltpu.make_async_copy(source, target, sems.at[at])
        for at, (source, target) in enumerate(moves)
    ]
    for copy in copies:
        copy.start()
    copies[0].wait()
    x = pair[...].astype(F32)
    centered = x - jnp.mean(x, axis=-1, keepdims=True)
    variance = jnp.mean(centered * centered, axis=-1, keepdims=True)
    normalized = centered * lax.rsqrt(variance + EPS)
    for copy in copies[1:]:
        copy.wait()
    normed = (normalized * gain[...] + bias[...]).astype(BF16)
    normed_out[...] = normed
    k_of_lane = lane_iota((16, 128)) & 15
    spread = (k_of_lane == lax.broadcasted_iota(jnp.int32, (16, 128), 0)).astype(BF16)
    masks = lax.dot_general(
        mask[...].astype(F32).astype(BF16),
        spread,
        (((0,), (0,)), ((), ())),
        preferred_element_type=F32,
    )
    own_row = (lane_iota((8, 128)) >> 4) == lax.broadcasted_iota(jnp.int32, (8, 128), 0)
    for q in range(4):
        projected = lax.dot_general(
            weight[...],
            normed[q * 128 : (q + 1) * 128],
            (((0,), (1,)), ((), ())),
            preferred_element_type=F32,
        )
        keep = jnp.sum(jnp.where(own_row, masks[q * 8 : (q + 1) * 8], 0.0), axis=0, keepdims=True)
        rows[pl.ds(q * 2, 128, stride=8), :] = (
            jax.nn.sigmoid(projected[:128]) * projected[128:256] * keep
        )
        rows[pl.ds(q * 2 + 1, 128, stride=8), :] = (
            jax.nn.sigmoid(projected[256:384]) * projected[384:] * keep
        )
    sent[...] = rows[...].astype(BF16)


def sides_kernel(got, left, right, rows):
    rows[...] = got[...].astype(F32)
    for side, target in enumerate((left, right)):
        for g_hi in range(4):
            pieces = [
                rows[pl.ds((g_hi * 8 + g) * 32 + side, 16, stride=2), :] for g in range(8)
            ]
            pieces = swap_bits(pieces, ((0, 4), (1, 5), (2, 6)))
            for r in range(8):
                target[pl.ds(r * 16, 16), pl.ds(g_hi * 128, 128)] = pieces[r].astype(BF16)


def triangle_kernel(right, left, sent, product, rows):
    product[...] = lax.dot_general(
        right[...], left[...], (((1,), (1,)), ((), ())), preferred_element_type=F32
    )
    for zh in range(4):
        for jh in range(2):
            pieces = [product[pl.ds(zh * 128 + r * 16 + jh, 8, stride=2), :] for r in range(8)]
            pieces = swap_bits(pieces, ((0, 2), (1, 3)))
            for v in range(8):
                high, owner_row = v >> 2, v & 3
                for yh in range(2):
                    at = ((yh * 16 + zh * 4) * 4 + owner_row) * 4 + jh * 2 + high
                    rows[pl.ds(at, 4, stride=16), :] = pieces[v][yh * 4 : yh * 4 + 4]
    sent[...] = rows[...].astype(BF16)


def mix_kernel(
    got, normed, gate_weight, scales, out_weight, update, rows, mixed, ordered, staged, sems
):
    rows[...] = got[...].astype(F32)
    gains = jnp.broadcast_to(scales[0:1, :], (128, 128)).T
    biases = jnp.broadcast_to(scales[1:2, :], (128, 128)).T
    for h in range(4):
        triangle = rows[pl.ds(h, 128, stride=4), :]
        centered = triangle - jnp.mean(triangle, axis=0, keepdims=True)
        variance = jnp.mean(centered * centered, axis=0, keepdims=True)
        tri_normed = (centered * lax.rsqrt(variance + EPS) * gains + biases).astype(BF16)
        mixed[pl.ds(h * 128, 128), :] = lax.dot_general(
            tri_normed, out_weight[...], (((0,), (0,)), ((), ())), preferred_element_type=F32
        )
    copies = []
    for s in range(4):
        block = pl.ds(s * 128, 128)
        gating = jax.nn.sigmoid(
            jnp.dot(normed[block, :], gate_weight[...], preferred_element_type=F32)
        )
        for h in range(4):
            for jj in range(4):
                ordered[pl.ds(s * 128 + h * 4 + jj, 8, stride=16), :] = mixed[
                    pl.ds(h * 128 + jj * 4 + s, 8, stride=16), :
                ]
        staged[block, :] = (ordered[block, :] * gating).astype(BF16)
        copies.append(pltpu.make_async_copy(staged.at[block], update.at[block], sems.at[s]))
        copies[s].start()
    for copy in copies:
        copy.wait()


def local_call(kernel, outs, scratch=(), in_space=pltpu.VMEM, out_space=pltpu.VMEM):

    def call(*args):
        return pl.pallas_call(
            kernel,
            out_shape=outs,
            in_specs=[pl.BlockSpec(memory_space=in_space)] * len(args),
            out_specs=jax.tree.map(lambda _: pl.BlockSpec(memory_space=out_space), outs),
            scratch_shapes=scratch,
            compiler_params=pltpu.CompilerParams(vmem_limit_bytes=16 << 20),
            cost_estimate=pl.CostEstimate(
                flops=1_000_000, bytes_accessed=1 << 20, transcendentals=0
            ),
        )(*args)

    return call


def on_device(
    pair, pair_mask, in_gain, in_bias, proj_weight, gate_weight, out_gain, out_bias, out_weight
):
    shape = jax.ShapeDtypeStruct
    inputs = (
        pair.reshape(512, 128),
        proj_weight,
        pair_mask.T,
        in_gain[None],
        in_bias[None],
        out_gain[None],
        out_bias[None],
    )
    sent, normed, scales = local_call(
        project_kernel,
        (shape((1024, 128), BF16), shape((512, 128), BF16), shape((2, 128), F32)),
        [
            pltpu.VMEM((512, 128), BF16),
            pltpu.VMEM((128, 512), BF16),
            pltpu.VMEM((16, 32), jnp.int32),
            pltpu.VMEM((1, 128), F32),
            pltpu.VMEM((1, 128), F32),
            pltpu.VMEM((1024, 128), F32),
            pltpu.SemaphoreType.DMA((7,)),
        ],
        in_space=pltpu.HBM,
    )(*(pltpu.with_memory_space_constraint(a, pltpu.HBM) for a in inputs))
    got = lax.all_to_all(sent.reshape(128, 8, 128), ORDER, 0, 0, tiled=True)
    left, right = local_call(
        sides_kernel,
        (shape((128, 512), BF16), shape((128, 512), BF16)),
        [pltpu.VMEM((1024, 128), F32)],
    )(got.reshape(1024, 128))
    every_right = lax.all_gather(right, "zh", axis=0, tiled=True)
    sums = local_call(
        triangle_kernel,
        shape((512, 128), BF16),
        [pltpu.VMEM((512, 128), F32), pltpu.VMEM((512, 128), F32)],
    )(every_right, left)
    back = lax.all_to_all(sums.reshape(128, 4, 128), ORDER, 0, 0, tiled=True)
    block = pltpu.VMEM((512, 128), F32)
    update = local_call(
        mix_kernel,
        shape((512, 128), BF16),
        [block, block, block, pltpu.VMEM((512, 128), BF16), pltpu.SemaphoreType.DMA((4,))],
        out_space=pltpu.HBM,
    )(back.reshape(512, 128), normed, gate_weight, scales, out_weight)
    return update.reshape(32, 16, 128)


def solution(mesh):
    finer = Mesh(mesh.devices.reshape((2, 4) + (2,) * 6), ROW_AXES + COLUMN_AXES)
    in_specs = (
        P(ROW_AXES, COLUMN_AXES, None),
        P(ROW_AXES, COLUMN_AXES),
        P(),
        P(),
        P(),
        P(),
        P(),
        P(),
        P(),
    )
    return jax.shard_map(
        on_device,
        mesh=finer,
        in_specs=in_specs,
        out_specs=P(ROW_AXES, COLUMN_AXES, None),
        check_vma=False,
    )
```

```python
import jax
import jax.numpy as jnp
from jax import lax
from jax.experimental import pallas as pl
from jax.experimental.pallas import tpu as pltpu
from jax.sharding import Mesh
from jax.sharding import PartitionSpec as P

ROW_AXES = ("yh", "z2", "z1", "z0")
COLUMN_AXES = ("y1", "y0", "x1", "x0", "co")
ORDER = ("y1", "y0", "co", "z1", "z0", "yh", "z2")
EPS = 1e-05
F32 = jnp.float32
BF16 = jnp.bfloat16


def lane_iota(shape):
    return lax.broadcasted_iota(jnp.int32, shape, len(shape) - 1)


def swap_bits(arrays, bits):
    arrays = list(arrays)
    lanes = lane_iota(arrays[0].shape)
    for pos, lane in bits:
        step, width = 1 << pos, 1 << lane
        high = (lanes & width) != 0
        for at in range(len(arrays)):
            if at & step:
                continue
            a, b = arrays[at], arrays[at + step]
            arrays[at] = jnp.where(high, pltpu.roll(b, width, 1), a)
            arrays[at + step] = jnp.where(high, b, pltpu.roll(a, 128 - width, 1))
    return arrays


def project_kernel(
    pair_hbm,
    weight_hbm,
    mask_hbm,
    gain_hbm,
    bias_hbm,
    out_gain_hbm,
    out_bias_hbm,
    sent,
    normed_out,
    scales,
    pair,
    weight,
    mask,
    gain,
    bias,
    rows,
    sems,
):
    moves = (
        (pair_hbm, pair),
        (gain_hbm, gain),
        (bias_hbm, bias),
        (weight_hbm, weight),
        (mask_hbm, mask),
        (out_gain_hbm, scales.at[pl.ds(0, 1)]),
        (out_bias_hbm, scales.at[pl.ds(1, 1)]),
    )
    copies = [
        pltpu.make_async_copy(source, target, sems.at[at])
        for at, (source, target) in enumerate(moves)
    ]
    for copy in copies:
        copy.start()
    copies[0].wait()
    x = pair[...].astype(F32)
    centered = x - jnp.mean(x, axis=-1, keepdims=True)
    variance = jnp.mean(centered * centered, axis=-1, keepdims=True)
    normalized = centered * lax.rsqrt(variance + EPS)
    for copy in copies[1:]:
        copy.wait()
    normed = (normalized * gain[...] + bias[...]).astype(BF16)
    normed_out[...] = normed
    k_of_lane = lane_iota((16, 128)) & 15
    spread = (k_of_lane == lax.broadcasted_iota(jnp.int32, (16, 128), 0)).astype(BF16)
    masks = lax.dot_general(
        mask[...].astype(F32).astype(BF16),
        spread,
        (((0,), (0,)), ((), ())),
        preferred_element_type=F32,
    )
    own_row = (lane_iota((8, 128)) >> 4) == lax.broadcasted_iota(jnp.int32, (8, 128), 0)
    for q in range(4):
        projected = lax.dot_general(
            weight[...],
            normed[q * 128 : (q + 1) * 128],
            (((0,), (1,)), ((), ())),
            preferred_element_type=F32,
        )
        keep = jnp.sum(jnp.where(own_row, masks[q * 8 : (q + 1) * 8], 0.0), axis=0, keepdims=True)
        rows[pl.ds(q * 2, 128, stride=8), :] = (
            jax.nn.sigmoid(projected[:128]) * projected[128:256] * keep
        )
        rows[pl.ds(q * 2 + 1, 128, stride=8), :] = (
            jax.nn.sigmoid(projected[256:384]) * projected[384:] * keep
        )
    sent[...] = rows[...].astype(BF16)


def partial_kernel(got, sent, left, right, rows):
    rows[...] = got[...].astype(F32)
    for side, target in enumerate((left, right)):
        for z in range(4):
            pieces = [rows[pl.ds(g * 128 + z * 32 + side, 16, stride=2), :] for g in range(8)]
            pieces = swap_bits(pieces, ((0, 4), (1, 5), (2, 6)))
            for r in range(8):
                target[pl.ds(z * 128 + r * 16, 16), :] = pieces[r].astype(BF16)
    for z in range(4):
        block = pl.ds(z * 128, 128)
        sent[block, :] = lax.dot_general(
            right[block, :], left[...], (((1,), (1,)), ((), ())), preferred_element_type=F32
        ).astype(BF16)


def sum_kernel(got, sent, total, rows):
    for z in range(4):
        lanes = pl.ds(z * 128, 128)
        total[lanes, :] = sum(got[pl.ds(x * 128, 128), lanes].astype(F32) for x in range(4))
        for jh in range(2):
            pieces = [total[pl.ds(z * 128 + r * 16 + jh, 8, stride=2), :] for r in range(8)]
            pieces = swap_bits(pieces, ((0, 2), (1, 3)))
            for v in range(8):
                at = (z * 4 + (v & 3)) * 4 + jh * 2 + (v >> 2)
                rows[pl.ds(at, 8, stride=64), :] = pieces[v]
    sent[...] = rows[...].astype(BF16)


def mix_kernel(
    got, normed, gate_weight, scales, out_weight, update, rows, mixed, ordered, staged, sems
):
    rows[...] = got[...].astype(F32)
    gains = jnp.broadcast_to(scales[0:1, :], (128, 128)).T
    biases = jnp.broadcast_to(scales[1:2, :], (128, 128)).T
    for h in range(4):
        triangle = rows[pl.ds(h, 128, stride=4), :]
        centered = triangle - jnp.mean(triangle, axis=0, keepdims=True)
        variance = jnp.mean(centered * centered, axis=0, keepdims=True)
        tri_normed = (centered * lax.rsqrt(variance + EPS) * gains + biases).astype(BF16)
        mixed[pl.ds(h * 128, 128), :] = lax.dot_general(
            tri_normed, out_weight[...], (((0,), (0,)), ((), ())), preferred_element_type=F32
        )
    copies = []
    for s in range(4):
        block = pl.ds(s * 128, 128)
        gating = jax.nn.sigmoid(
            jnp.dot(normed[block, :], gate_weight[...], preferred_element_type=F32)
        )
        for h in range(4):
            for jj in range(4):
                ordered[pl.ds(s * 128 + h * 4 + jj, 8, stride=16), :] = mixed[
                    pl.ds(h * 128 + jj * 4 + s, 8, stride=16), :
                ]
        staged[block, :] = (ordered[block, :] * gating).astype(BF16)
        copies.append(pltpu.make_async_copy(staged.at[block], update.at[block], sems.at[s]))
        copies[s].start()
    for copy in copies:
        copy.wait()


def local_call(kernel, outs, scratch=(), in_space=pltpu.VMEM, out_space=pltpu.VMEM):

    def call(*args):
        return pl.pallas_call(
            kernel,
            out_shape=outs,
            in_specs=[pl.BlockSpec(memory_space=in_space)] * len(args),
            out_specs=jax.tree.map(lambda _: pl.BlockSpec(memory_space=out_space), outs),
            scratch_shapes=scratch,
            compiler_params=pltpu.CompilerParams(vmem_limit_bytes=16 << 20),
            cost_estimate=pl.CostEstimate(
                flops=1_000_000, bytes_accessed=1 << 20, transcendentals=0
            ),
        )(*args)

    return call


def on_device(
    pair, pair_mask, in_gain, in_bias, proj_weight, gate_weight, out_gain, out_bias, out_weight
):
    shape = jax.ShapeDtypeStruct
    inputs = (
        pair.reshape(512, 128),
        proj_weight,
        pair_mask.T,
        in_gain[None],
        in_bias[None],
        out_gain[None],
        out_bias[None],
    )
    sent, normed, scales = local_call(
        project_kernel,
        (shape((1024, 128), BF16), shape((512, 128), BF16), shape((2, 128), F32)),
        [
            pltpu.VMEM((512, 128), BF16),
            pltpu.VMEM((128, 512), BF16),
            pltpu.VMEM((16, 32), jnp.int32),
            pltpu.VMEM((1, 128), F32),
            pltpu.VMEM((1, 128), F32),
            pltpu.VMEM((1024, 128), F32),
            pltpu.SemaphoreType.DMA((7,)),
        ],
        in_space=pltpu.HBM,
    )(*(pltpu.with_memory_space_constraint(a, pltpu.HBM) for a in inputs))
    got = lax.all_to_all(sent.reshape(128, 8, 128), ORDER, 0, 0, tiled=True)
    side = pltpu.VMEM((512, 128), BF16)
    partial = local_call(
        partial_kernel, shape((512, 512), BF16), [side, side, pltpu.VMEM((1024, 128), F32)]
    )(got.reshape(1024, 128))
    parts = lax.all_to_all(partial.reshape(4, 128, 512), ("x1", "x0"), 0, 0, tiled=True)
    sums = local_call(
        sum_kernel,
        shape((512, 128), BF16),
        [pltpu.VMEM((512, 128), F32), pltpu.VMEM((512, 128), F32)],
    )(parts.reshape(512, 512))
    back = lax.all_to_all(sums.reshape(128, 4, 128), ORDER, 0, 0, tiled=True)
    block = pltpu.VMEM((512, 128), F32)
    update = local_call(
        mix_kernel,
        shape((512, 128), BF16),
        [block, block, block, pltpu.VMEM((512, 128), BF16), pltpu.SemaphoreType.DMA((4,))],
        out_space=pltpu.HBM,
    )(back.reshape(512, 128), normed, gate_weight, scales, out_weight)
    return update.reshape(32, 16, 128)


def solution(mesh):
    finer = Mesh(mesh.devices.reshape((2,) * 9), ROW_AXES + COLUMN_AXES)
    in_specs = (
        P(ROW_AXES, COLUMN_AXES, None),
        P(ROW_AXES, COLUMN_AXES),
        P(),
        P(),
        P(),
        P(),
        P(),
        P(),
        P(),
    )
    return jax.shard_map(
        on_device,
        mesh=finer,
        in_specs=in_specs,
        out_specs=P(ROW_AXES, COLUMN_AXES, None),
        check_vma=False,
    )
```

```python
import jax
import jax.numpy as jnp
from jax import lax
from jax.experimental import pallas as pl
from jax.experimental.pallas import tpu as pltpu
from jax.sharding import Mesh
from jax.sharding import PartitionSpec as P

ROW_AXES = ("yh", "z2", "z1", "z0")
COLUMN_AXES = ("y1", "y0", "x1", "x0", "co")
ORDER = ("y1", "y0", "co", "z1", "z0", "yh", "z2")
EPS = 1e-05
F32 = jnp.float32
BF16 = jnp.bfloat16


def lane_iota(shape):
    return lax.broadcasted_iota(jnp.int32, shape, len(shape) - 1)


def swap_bits(arrays, bits):
    arrays = list(arrays)
    lanes = lane_iota(arrays[0].shape)
    for pos, lane in bits:
        step, width = 1 << pos, 1 << lane
        high = (lanes & width) != 0
        for at in range(len(arrays)):
            if at & step:
                continue
            a, b = arrays[at], arrays[at + step]
            arrays[at] = jnp.where(high, pltpu.roll(b, width, 1), a)
            arrays[at + step] = jnp.where(high, b, pltpu.roll(a, 128 - width, 1))
    return arrays


def project_kernel(
    pair_hbm,
    weight_hbm,
    mask_hbm,
    gain_hbm,
    bias_hbm,
    out_gain_hbm,
    out_bias_hbm,
    sent,
    normed_out,
    scales,
    pair,
    weight,
    mask,
    gain,
    bias,
    rows,
    sems,
):
    quarters = [pl.ds(q * 128, 128) for q in range(4)]
    moves = (
        *((pair_hbm.at[q], pair.at[q]) for q in quarters),
        (gain_hbm, gain),
        (bias_hbm, bias),
        *((weight_hbm.at[:, q], weight.at[:, q]) for q in quarters),
        (mask_hbm, mask),
        (out_gain_hbm, scales.at[pl.ds(0, 1)]),
        (out_bias_hbm, scales.at[pl.ds(1, 1)]),
    )
    copies = [
        pltpu.make_async_copy(source, target, sems.at[at])
        for at, (source, target) in enumerate(moves)
    ]
    for copy in copies:
        copy.start()
    normalized = []
    for q in range(4):
        copies[q].wait()
        x = pair[quarters[q], :].astype(F32)
        centered = x - jnp.mean(x, axis=-1, keepdims=True)
        variance = jnp.mean(centered * centered, axis=-1, keepdims=True)
        normalized.append(centered * lax.rsqrt(variance + EPS))
    for copy in copies[4:]:
        copy.wait()
    normed = [(part * gain[...] + bias[...]).astype(BF16) for part in normalized]
    for q in range(4):
        normed_out[quarters[q], :] = normed[q]
    k_of_lane = lane_iota((16, 128)) & 15
    spread = (k_of_lane == lax.broadcasted_iota(jnp.int32, (16, 128), 0)).astype(BF16)
    masks = lax.dot_general(
        mask[...].astype(F32).astype(BF16),
        spread,
        (((0,), (0,)), ((), ())),
        preferred_element_type=F32,
    )
    own_row = (lane_iota((8, 128)) >> 4) == lax.broadcasted_iota(jnp.int32, (8, 128), 0)
    for q in range(4):
        projected = lax.dot_general(
            weight[...],
            normed[q],
            (((0,), (1,)), ((), ())),
            preferred_element_type=F32,
        )
        keep = jnp.sum(jnp.where(own_row, masks[q * 8 : (q + 1) * 8], 0.0), axis=0, keepdims=True)
        rows[pl.ds(q * 2, 128, stride=8), :] = (
            jax.nn.sigmoid(projected[:128]) * projected[128:256] * keep
        )
        rows[pl.ds(q * 2 + 1, 128, stride=8), :] = (
            jax.nn.sigmoid(projected[256:384]) * projected[384:] * keep
        )
    sent[...] = rows[...].astype(BF16)


def partial_kernel(got, sent, left, right, rows):
    rows[...] = got[...].astype(F32)
    for side, target in enumerate((left, right)):
        for z in range(4):
            pieces = [rows[pl.ds(g * 128 + z * 32 + side, 16, stride=2), :] for g in range(8)]
            pieces = swap_bits(pieces, ((0, 4), (1, 5), (2, 6)))
            for r in range(8):
                target[pl.ds(z * 128 + r * 16, 16), :] = pieces[r].astype(BF16)
    for z in range(4):
        sums = lax.dot_general(
            right[pl.ds(z * 128, 128), :],
            left[...],
            (((1,), (1,)), ((), ())),
            preferred_element_type=F32,
        )
        sent[pl.ds((z % 2 * 2 + z // 2) * 128, 128), :] = sums.astype(BF16)


def sum_kernel(got, sent, total, rows):
    for z in range(4):
        lanes = pl.ds(z * 128, 128)
        total[lanes, :] = sum(got[pl.ds(x * 128, 128), lanes].astype(F32) for x in range(4))
        for jh in range(2):
            pieces = [total[pl.ds(z * 128 + r * 16 + jh, 8, stride=2), :] for r in range(8)]
            pieces = swap_bits(pieces, ((0, 2), (1, 3)))
            for v in range(8):
                at = (z * 4 + (v & 3)) * 4 + jh * 2 + (v >> 2)
                rows[pl.ds(at, 8, stride=64), :] = pieces[v]
    sent[...] = rows[...].astype(BF16)


def mix_kernel(
    got, normed, gate_weight, scales, out_weight, update, rows, mixed, ordered, staged, sems
):
    rows[...] = got[...].astype(F32)
    gains = jnp.broadcast_to(scales[0:1, :], (128, 128)).T
    biases = jnp.broadcast_to(scales[1:2, :], (128, 128)).T
    for h in range(4):
        triangle = rows[pl.ds(h, 128, stride=4), :]
        centered = triangle - jnp.mean(triangle, axis=0, keepdims=True)
        variance = jnp.mean(centered * centered, axis=0, keepdims=True)
        tri_normed = (centered * lax.rsqrt(variance + EPS) * gains + biases).astype(BF16)
        mixed[pl.ds(h * 128, 128), :] = lax.dot_general(
            tri_normed, out_weight[...], (((0,), (0,)), ((), ())), preferred_element_type=F32
        )
    copies = []
    for s in range(4):
        block = pl.ds(s * 128, 128)
        gating = jax.nn.sigmoid(
            jnp.dot(normed[block, :], gate_weight[...], preferred_element_type=F32)
        )
        for h in range(4):
            for jj in range(4):
                ordered[pl.ds(s * 128 + h * 4 + jj, 8, stride=16), :] = mixed[
                    pl.ds(h * 128 + jj * 4 + s, 8, stride=16), :
                ]
        staged[block, :] = (ordered[block, :] * gating).astype(BF16)
        copies.append(pltpu.make_async_copy(staged.at[block], update.at[block], sems.at[s]))
        copies[s].start()
    for copy in copies:
        copy.wait()


def local_call(kernel, outs, scratch=(), in_space=pltpu.VMEM, out_space=pltpu.VMEM):

    def call(*args):
        return pl.pallas_call(
            kernel,
            out_shape=outs,
            in_specs=[pl.BlockSpec(memory_space=in_space)] * len(args),
            out_specs=jax.tree.map(lambda _: pl.BlockSpec(memory_space=out_space), outs),
            scratch_shapes=scratch,
            compiler_params=pltpu.CompilerParams(vmem_limit_bytes=16 << 20),
            cost_estimate=pl.CostEstimate(
                flops=1_000_000, bytes_accessed=1 << 20, transcendentals=0
            ),
        )(*args)

    return call


def on_device(
    pair, pair_mask, in_gain, in_bias, proj_weight, gate_weight, out_gain, out_bias, out_weight
):
    shape = jax.ShapeDtypeStruct
    inputs = (
        pair.reshape(512, 128),
        proj_weight,
        pair_mask.T,
        in_gain[None],
        in_bias[None],
        out_gain[None],
        out_bias[None],
    )
    sent, normed, scales = local_call(
        project_kernel,
        (shape((1024, 128), BF16), shape((512, 128), BF16), shape((2, 128), F32)),
        [
            pltpu.VMEM((512, 128), BF16),
            pltpu.VMEM((128, 512), BF16),
            pltpu.VMEM((16, 32), jnp.int32),
            pltpu.VMEM((1, 128), F32),
            pltpu.VMEM((1, 128), F32),
            pltpu.VMEM((1024, 128), F32),
            pltpu.SemaphoreType.DMA((13,)),
        ],
        in_space=pltpu.HBM,
    )(*(pltpu.with_memory_space_constraint(a, pltpu.HBM) for a in inputs))
    got = lax.all_to_all(sent.reshape(128, 8, 128), ORDER, 0, 0, tiled=True)
    side = pltpu.VMEM((512, 128), BF16)
    partial = local_call(
        partial_kernel, shape((512, 512), BF16), [side, side, pltpu.VMEM((1024, 128), F32)]
    )(got.reshape(1024, 128))
    parts = lax.all_to_all(partial.reshape(4, 128, 512), ("x0", "x1"), 0, 0, tiled=True)
    sums = local_call(
        sum_kernel,
        shape((512, 128), BF16),
        [pltpu.VMEM((512, 128), F32), pltpu.VMEM((512, 128), F32)],
    )(parts.reshape(512, 512))
    back = lax.all_to_all(sums.reshape(128, 4, 128), ORDER, 0, 0, tiled=True)
    block = pltpu.VMEM((512, 128), F32)
    update = local_call(
        mix_kernel,
        shape((512, 128), BF16),
        [block, block, block, pltpu.VMEM((512, 128), BF16), pltpu.SemaphoreType.DMA((4,))],
        out_space=pltpu.HBM,
    )(back.reshape(512, 128), normed, gate_weight, scales, out_weight)
    return update.reshape(32, 16, 128)


def solution(mesh):
    finer = Mesh(mesh.devices.reshape((2,) * 9), ROW_AXES + COLUMN_AXES)
    in_specs = (
        P(ROW_AXES, COLUMN_AXES, None),
        P(ROW_AXES, COLUMN_AXES),
        P(),
        P(),
        P(),
        P(),
        P(),
        P(),
        P(),
    )
    return jax.shard_map(
        on_device,
        mesh=finer,
        in_specs=in_specs,
        out_specs=P(ROW_AXES, COLUMN_AXES, None),
        check_vma=False,
    )
```

```python
import jax
import jax.numpy as jnp
from jax import lax
from jax.experimental import pallas as pl
from jax.experimental.pallas import tpu as pltpu
from jax.sharding import Mesh
from jax.sharding import PartitionSpec as P

ROW_AXES = ("yh", "z2", "z1", "z0")
COLUMN_AXES = ("y1", "y0", "x1", "x0", "co")
ORDER = ("y1", "y0", "co", "z1", "z0", "yh", "z2")
BACK_ORDER = ("y1", "y0", "z1", "z0", "yh", "z2")
EPS = 1e-05
F32 = jnp.float32
BF16 = jnp.bfloat16


def lane_iota(shape):
    return lax.broadcasted_iota(jnp.int32, shape, len(shape) - 1)


def swap_bits(arrays, bits):
    arrays = list(arrays)
    lanes = lane_iota(arrays[0].shape)
    for pos, lane in bits:
        step, width = 1 << pos, 1 << lane
        high = (lanes & width) != 0
        for at in range(len(arrays)):
            if at & step:
                continue
            a, b = arrays[at], arrays[at + step]
            arrays[at] = jnp.where(high, pltpu.roll(b, width, 1), a)
            arrays[at + step] = jnp.where(high, b, pltpu.roll(a, 128 - width, 1))
    return arrays


def project_kernel(
    pair_hbm,
    weight_hbm,
    mask_hbm,
    gain_hbm,
    bias_hbm,
    out_gain_hbm,
    out_bias_hbm,
    sent,
    normed_out,
    scales,
    pair,
    weight,
    mask,
    gain,
    bias,
    rows,
    sems,
):
    moves = (
        (pair_hbm, pair),
        (gain_hbm, gain),
        (bias_hbm, bias),
        (weight_hbm, weight),
        (mask_hbm, mask),
        (out_gain_hbm, scales.at[pl.ds(0, 1)]),
        (out_bias_hbm, scales.at[pl.ds(1, 1)]),
    )
    copies = [
        pltpu.make_async_copy(source, target, sems.at[at])
        for at, (source, target) in enumerate(moves)
    ]
    for copy in copies:
        copy.start()
    copies[0].wait()
    x = pair[...].astype(F32)
    centered = x - jnp.mean(x, axis=-1, keepdims=True)
    variance = jnp.mean(centered * centered, axis=-1, keepdims=True)
    normalized = centered * lax.rsqrt(variance + EPS)
    for copy in copies[1:]:
        copy.wait()
    normed = (normalized * gain[...] + bias[...]).astype(BF16)
    normed_out[...] = normed
    k_of_lane = lane_iota((16, 128)) & 15
    spread = (k_of_lane == lax.broadcasted_iota(jnp.int32, (16, 128), 0)).astype(BF16)
    masks = lax.dot_general(
        mask[...].astype(F32).astype(BF16),
        spread,
        (((0,), (0,)), ((), ())),
        preferred_element_type=F32,
    )
    own_row = (lane_iota((8, 128)) >> 4) == lax.broadcasted_iota(jnp.int32, (8, 128), 0)
    for q in range(4):
        projected = lax.dot_general(
            weight[...],
            normed[q * 128 : (q + 1) * 128],
            (((0,), (1,)), ((), ())),
            preferred_element_type=F32,
        )
        keep = jnp.sum(jnp.where(own_row, masks[q * 8 : (q + 1) * 8], 0.0), axis=0, keepdims=True)
        rows[pl.ds(q * 2, 128, stride=8), :] = (
            jax.nn.sigmoid(projected[:128]) * projected[128:256] * keep
        )
        rows[pl.ds((q % 2 * 2 + q // 2) * 2 + 1, 128, stride=8), :] = (
            jax.nn.sigmoid(projected[256:384]) * projected[384:] * keep
        )
    sent[...] = rows[...].astype(BF16)


def residues_in_lanes(rows, start, size, stride):
    pieces = [rows[pl.ds(start + g * 128, size, stride=stride), :] for g in range(8)]
    return swap_bits(pieces, ((0, 4), (1, 5), (2, 6)))


def partial_kernel(got, sent, left, right, rows):
    rows[...] = got[...].astype(F32)
    for z in range(4):
        for r, piece in enumerate(residues_in_lanes(rows, z * 32, 16, 2)):
            left[pl.ds(z * 128 + r * 16, 16), :] = piece.astype(BF16)
        for core in range(2):
            pieces = residues_in_lanes(rows, z * 32 + core * 2 + 1, 8, 4)
            for r in range(0, 8, 2):
                both = jnp.concatenate(pieces[r : r + 2], axis=0)
                right[pl.ds(z * 128 + core * 64 + r * 8, 16), :] = both.astype(BF16)
    for z in range(4):
        block = pl.ds(z * 128, 128)
        sent[block, :] = lax.dot_general(
            right[block, :], left[...], (((1,), (1,)), ((), ())), preferred_element_type=F32
        ).astype(BF16)


def sum_kernel(got, sent, total, rows):
    for core in range(2):
        for z in range(4):
            base = (core * 4 + z) * 64
            total[pl.ds(base, 64), :] = sum(
                got[pl.ds((x * 2 + core) * 64, 64), pl.ds(z * 128, 128)].astype(F32)
                for x in range(4)
            )
            for jh in range(2):
                pieces = [total[pl.ds(base + t * 16 + jh, 8, stride=2), :] for t in range(4)]
                pieces = swap_bits(pieces, ((0, 2), (1, 3)))
                for v in range(4):
                    for low in range(2):
                        at = (z * 4 + v) * 8 + core * 4 + jh * 2 + low
                        rows[pl.ds(at, 4, stride=128), :] = pieces[v][low * 4 : low * 4 + 4]
    sent[...] = rows[0:512, :].astype(BF16)


def mix_kernel(
    got, normed, gate_weight, scales, out_weight, update, rows, mixed, ordered, staged, sems
):
    rows[...] = got[...].astype(F32)
    gains = jnp.broadcast_to(scales[0:1, :], (128, 128)).T
    biases = jnp.broadcast_to(scales[1:2, :], (128, 128)).T
    for h in range(4):
        triangle = jnp.concatenate(
            [
                rows[pl.ds(y * 128 + core * 4 + h, 16, stride=8), :]
                for y in range(4)
                for core in range(2)
            ],
            axis=0,
        )
        centered = triangle - jnp.mean(triangle, axis=0, keepdims=True)
        variance = jnp.mean(centered * centered, axis=0, keepdims=True)
        tri_normed = (centered * lax.rsqrt(variance + EPS) * gains + biases).astype(BF16)
        mixed[pl.ds(h * 128, 128), :] = lax.dot_general(
            tri_normed, out_weight[...], (((0,), (0,)), ((), ())), preferred_element_type=F32
        )
    copies = []
    for s in range(4):
        block = pl.ds(s * 128, 128)
        gating = jax.nn.sigmoid(
            jnp.dot(normed[block, :], gate_weight[...], preferred_element_type=F32)
        )
        for h in range(4):
            for jj in range(4):
                column = h // 2 * 8 + jj * 2 + h % 2
                ordered[pl.ds(s * 128 + column, 8, stride=16), :] = mixed[
                    pl.ds(h * 128 + jj * 4 + s, 8, stride=16), :
                ]
        staged[block, :] = (ordered[block, :] * gating).astype(BF16)
        copies.append(pltpu.make_async_copy(staged.at[block], update.at[block], sems.at[s]))
        copies[s].start()
    for copy in copies:
        copy.wait()


def local_call(kernel, outs, scratch=(), in_space=pltpu.VMEM, out_space=pltpu.VMEM):

    def call(*args):
        return pl.pallas_call(
            kernel,
            out_shape=outs,
            in_specs=[pl.BlockSpec(memory_space=in_space)] * len(args),
            out_specs=jax.tree.map(lambda _: pl.BlockSpec(memory_space=out_space), outs),
            scratch_shapes=scratch,
            compiler_params=pltpu.CompilerParams(vmem_limit_bytes=16 << 20),
            cost_estimate=pl.CostEstimate(
                flops=1_000_000, bytes_accessed=1 << 20, transcendentals=0
            ),
        )(*args)

    return call


def on_device(
    pair, pair_mask, in_gain, in_bias, proj_weight, gate_weight, out_gain, out_bias, out_weight
):
    shape = jax.ShapeDtypeStruct
    inputs = (
        pair.reshape(512, 128),
        proj_weight,
        pair_mask.T,
        in_gain[None],
        in_bias[None],
        out_gain[None],
        out_bias[None],
    )
    sent, normed, scales = local_call(
        project_kernel,
        (shape((1024, 128), BF16), shape((512, 128), BF16), shape((2, 128), F32)),
        [
            pltpu.VMEM((512, 128), BF16),
            pltpu.VMEM((128, 512), BF16),
            pltpu.VMEM((16, 32), jnp.int32),
            pltpu.VMEM((1, 128), F32),
            pltpu.VMEM((1, 128), F32),
            pltpu.VMEM((1024, 128), F32),
            pltpu.SemaphoreType.DMA((7,)),
        ],
        in_space=pltpu.HBM,
    )(*(pltpu.with_memory_space_constraint(a, pltpu.HBM) for a in inputs))
    got = lax.all_to_all(sent.reshape(128, 8, 128), ORDER, 0, 0, tiled=True)
    side = pltpu.VMEM((512, 128), BF16)
    partial = local_call(
        partial_kernel, shape((512, 512), BF16), [side, side, pltpu.VMEM((1024, 128), F32)]
    )(got.reshape(1024, 128))
    parts = lax.all_to_all(partial.reshape(8, 64, 512), ("x1", "x0", "co"), 0, 0, tiled=True)
    sums = local_call(
        sum_kernel,
        shape((512, 128), BF16),
        [pltpu.VMEM((512, 128), F32), pltpu.VMEM((1024, 128), F32)],
    )(parts.reshape(512, 512))
    back = lax.all_to_all(sums.reshape(64, 8, 128), BACK_ORDER, 0, 0, tiled=True)
    block = pltpu.VMEM((512, 128), F32)
    update = local_call(
        mix_kernel,
        shape((512, 128), BF16),
        [block, block, block, pltpu.VMEM((512, 128), BF16), pltpu.SemaphoreType.DMA((4,))],
        out_space=pltpu.HBM,
    )(back.reshape(512, 128), normed, gate_weight, scales, out_weight)
    return update.reshape(32, 16, 128)


def solution(mesh):
    finer = Mesh(mesh.devices.reshape((2,) * 9), ROW_AXES + COLUMN_AXES)
    in_specs = (
        P(ROW_AXES, COLUMN_AXES, None),
        P(ROW_AXES, COLUMN_AXES),
        P(),
        P(),
        P(),
        P(),
        P(),
        P(),
        P(),
    )
    return jax.shard_map(
        on_device,
        mesh=finer,
        in_specs=in_specs,
        out_specs=P(ROW_AXES, COLUMN_AXES, None),
        check_vma=False,
    )
```

```python
import jax
import jax.numpy as jnp
from jax import lax
from jax.experimental import pallas as pl
from jax.experimental.pallas import tpu as pltpu
from jax.sharding import Mesh
from jax.sharding import PartitionSpec as P

ROW_AXES = ("yh", "z2", "z1", "z0")
COLUMN_AXES = ("y1", "y0", "x1", "x0", "co")
ORDER = ("y1", "y0", "co", "z1", "z0", "yh", "z2")
BACK_ORDER = ("y1", "y0", "z1", "z0", "yh", "z2")
EPS = 1e-05
F32 = jnp.float32
BF16 = jnp.bfloat16


def lane_iota(shape):
    return lax.broadcasted_iota(jnp.int32, shape, len(shape) - 1)


def swap_bits(arrays, bits):
    arrays = list(arrays)
    lanes = lane_iota(arrays[0].shape)
    for pos, lane in bits:
        step, width = 1 << pos, 1 << lane
        high = (lanes & width) != 0
        for at in range(len(arrays)):
            if at & step:
                continue
            a, b = arrays[at], arrays[at + step]
            arrays[at] = jnp.where(high, pltpu.roll(b, width, 1), a)
            arrays[at + step] = jnp.where(high, b, pltpu.roll(a, 128 - width, 1))
    return arrays


def project_kernel(
    pair_hbm,
    weight_hbm,
    mask_hbm,
    gain_hbm,
    bias_hbm,
    out_gain_hbm,
    out_bias_hbm,
    sent,
    normed_out,
    scales,
    pair,
    weight,
    mask,
    gain,
    bias,
    rows,
    sems,
):
    halves = [(pl.ds(h * 256, 256), pl.ds(h * 64, 64)) for h in range(2)]
    moves = (
        *((pair_hbm.at[h], pair.at[h]) for h, _ in halves),
        *((weight_hbm.at[h], weight.at[h]) for _, h in halves),
        (gain_hbm, gain),
        (bias_hbm, bias),
        (mask_hbm, mask),
        (out_gain_hbm, scales.at[pl.ds(0, 1)]),
        (out_bias_hbm, scales.at[pl.ds(1, 1)]),
    )
    copies = [
        pltpu.make_async_copy(source, target, sems.at[at])
        for at, (source, target) in enumerate(moves)
    ]
    for copy in copies:
        copy.start()
    copies[0].wait()
    copies[1].wait()
    x = pair[...].astype(F32)
    centered = x - jnp.mean(x, axis=-1, keepdims=True)
    variance = jnp.mean(centered * centered, axis=-1, keepdims=True)
    normalized = centered * lax.rsqrt(variance + EPS)
    for copy in copies[2:]:
        copy.wait()
    normed = (normalized * gain[...] + bias[...]).astype(BF16)
    normed_out[...] = normed
    k_of_lane = lane_iota((16, 128)) & 15
    spread = (k_of_lane == lax.broadcasted_iota(jnp.int32, (16, 128), 0)).astype(BF16)
    masks = lax.dot_general(
        mask[...].astype(F32).astype(BF16),
        spread,
        (((0,), (0,)), ((), ())),
        preferred_element_type=F32,
    )
    own_row = (lane_iota((8, 128)) >> 4) == lax.broadcasted_iota(jnp.int32, (8, 128), 0)
    for q in range(4):
        projected = lax.dot_general(
            weight[...],
            normed[q * 128 : (q + 1) * 128],
            (((0,), (1,)), ((), ())),
            preferred_element_type=F32,
        )
        keep = jnp.sum(jnp.where(own_row, masks[q * 8 : (q + 1) * 8], 0.0), axis=0, keepdims=True)
        rows[pl.ds(q * 2, 128, stride=8), :] = (
            jax.nn.sigmoid(projected[:128]) * projected[128:256] * keep
        )
        rows[pl.ds((q % 2 * 2 + q // 2) * 2 + 1, 128, stride=8), :] = (
            jax.nn.sigmoid(projected[256:384]) * projected[384:] * keep
        )
    sent[...] = rows[...].astype(BF16)


def residues_in_lanes(rows, start, size, stride):
    pieces = [rows[pl.ds(start + g * 128, size, stride=stride), :] for g in range(8)]
    return swap_bits(pieces, ((0, 4), (1, 5), (2, 6)))


def partial_kernel(got, sent, left, right, rows):
    rows[...] = got[...].astype(F32)
    for z in range(4):
        for r, piece in enumerate(residues_in_lanes(rows, z * 32, 16, 2)):
            left[pl.ds(z * 128 + r * 16, 16), :] = piece.astype(BF16)
        for core in range(2):
            pieces = residues_in_lanes(rows, z * 32 + core * 2 + 1, 8, 4)
            for r in range(0, 8, 2):
                both = jnp.concatenate(pieces[r : r + 2], axis=0)
                right[pl.ds(z * 128 + core * 64 + r * 8, 16), :] = both.astype(BF16)
    for z in range(4):
        sums = lax.dot_general(
            right[pl.ds(z * 128, 128), :],
            left[...],
            (((1,), (1,)), ((), ())),
            preferred_element_type=F32,
        ).astype(BF16)
        for core in range(2):
            to = (core * 4 + z % 2 * 2 + z // 2) * 64
            sent[pl.ds(to, 64), :] = sums[core * 64 : core * 64 + 64]


def sum_kernel(got, sent, total, rows):
    for core in range(2):
        for z in range(4):
            base = (core * 4 + z) * 64
            total[pl.ds(base, 64), :] = sum(
                got[pl.ds((core * 4 + x) * 64, 64), pl.ds(z * 128, 128)].astype(F32)
                for x in range(4)
            )
            for jh in range(2):
                pieces = [total[pl.ds(base + t * 16 + jh, 8, stride=2), :] for t in range(4)]
                pieces = swap_bits(pieces, ((0, 2), (1, 3)))
                for v in range(4):
                    for low in range(2):
                        at = (z * 4 + v) * 8 + core * 4 + jh * 2 + low
                        rows[pl.ds(at, 4, stride=128), :] = pieces[v][low * 4 : low * 4 + 4]
    sent[...] = rows[0:512, :].astype(BF16)


def mix_kernel(
    got, normed, gate_weight, scales, out_weight, update, rows, mixed, ordered, staged, sems
):
    rows[...] = got[...].astype(F32)
    gains = jnp.broadcast_to(scales[0:1, :], (128, 128)).T
    biases = jnp.broadcast_to(scales[1:2, :], (128, 128)).T
    for h in range(4):
        triangle = jnp.concatenate(
            [
                rows[pl.ds(y * 128 + core * 4 + h, 16, stride=8), :]
                for y in range(4)
                for core in range(2)
            ],
            axis=0,
        )
        centered = triangle - jnp.mean(triangle, axis=0, keepdims=True)
        variance = jnp.mean(centered * centered, axis=0, keepdims=True)
        tri_normed = (centered * lax.rsqrt(variance + EPS) * gains + biases).astype(BF16)
        mixed[pl.ds(h * 128, 128), :] = lax.dot_general(
            tri_normed, out_weight[...], (((0,), (0,)), ((), ())), preferred_element_type=F32
        )
    copies = []
    for s in range(4):
        block = pl.ds(s * 128, 128)
        gating = jax.nn.sigmoid(
            jnp.dot(normed[block, :], gate_weight[...], preferred_element_type=F32)
        )
        for h in range(4):
            for jj in range(4):
                column = h // 2 * 8 + jj * 2 + h % 2
                ordered[pl.ds(s * 128 + column, 8, stride=16), :] = mixed[
                    pl.ds(h * 128 + jj * 4 + s, 8, stride=16), :
                ]
        staged[block, :] = (ordered[block, :] * gating).astype(BF16)
        copies.append(pltpu.make_async_copy(staged.at[block], update.at[block], sems.at[s]))
        copies[s].start()
    for copy in copies:
        copy.wait()


def local_call(kernel, outs, scratch=(), in_space=pltpu.VMEM, out_space=pltpu.VMEM):

    def call(*args):
        return pl.pallas_call(
            kernel,
            out_shape=outs,
            in_specs=[pl.BlockSpec(memory_space=in_space)] * len(args),
            out_specs=jax.tree.map(lambda _: pl.BlockSpec(memory_space=out_space), outs),
            scratch_shapes=scratch,
            compiler_params=pltpu.CompilerParams(vmem_limit_bytes=16 << 20),
            cost_estimate=pl.CostEstimate(
                flops=1_000_000, bytes_accessed=1 << 20, transcendentals=0
            ),
        )(*args)

    return call


def on_device(
    pair, pair_mask, in_gain, in_bias, proj_weight, gate_weight, out_gain, out_bias, out_weight
):
    shape = jax.ShapeDtypeStruct
    inputs = (
        pair.reshape(512, 128),
        proj_weight,
        pair_mask.T,
        in_gain[None],
        in_bias[None],
        out_gain[None],
        out_bias[None],
    )
    sent, normed, scales = local_call(
        project_kernel,
        (shape((1024, 128), BF16), shape((512, 128), BF16), shape((2, 128), F32)),
        [
            pltpu.VMEM((512, 128), BF16),
            pltpu.VMEM((128, 512), BF16),
            pltpu.VMEM((16, 32), jnp.int32),
            pltpu.VMEM((1, 128), F32),
            pltpu.VMEM((1, 128), F32),
            pltpu.VMEM((1024, 128), F32),
            pltpu.SemaphoreType.DMA((9,)),
        ],
        in_space=pltpu.HBM,
    )(*(pltpu.with_memory_space_constraint(a, pltpu.HBM) for a in inputs))
    got = lax.all_to_all(sent.reshape(128, 8, 128), ORDER, 0, 0, tiled=True)
    side = pltpu.VMEM((512, 128), BF16)
    partial = local_call(
        partial_kernel, shape((512, 512), BF16), [side, side, pltpu.VMEM((1024, 128), F32)]
    )(got.reshape(1024, 128))
    parts = lax.all_to_all(partial.reshape(8, 64, 512), ("co", "x0", "x1"), 0, 0, tiled=True)
    sums = local_call(
        sum_kernel,
        shape((512, 128), BF16),
        [pltpu.VMEM((512, 128), F32), pltpu.VMEM((1024, 128), F32)],
    )(parts.reshape(512, 512))
    back = lax.all_to_all(sums.reshape(64, 8, 128), BACK_ORDER, 0, 0, tiled=True)
    block = pltpu.VMEM((512, 128), F32)
    update = local_call(
        mix_kernel,
        shape((512, 128), BF16),
        [block, block, block, pltpu.VMEM((512, 128), BF16), pltpu.SemaphoreType.DMA((4,))],
        out_space=pltpu.HBM,
    )(back.reshape(512, 128), normed, gate_weight, scales, out_weight)
    return update.reshape(32, 16, 128)


def solution(mesh):
    finer = Mesh(mesh.devices.reshape((2,) * 9), ROW_AXES + COLUMN_AXES)
    in_specs = (
        P(ROW_AXES, COLUMN_AXES, None),
        P(ROW_AXES, COLUMN_AXES),
        P(),
        P(),
        P(),
        P(),
        P(),
        P(),
        P(),
    )
    return jax.shard_map(
        on_device,
        mesh=finer,
        in_specs=in_specs,
        out_specs=P(ROW_AXES, COLUMN_AXES, None),
        check_vma=False,
    )
```

```python
import jax
import jax.numpy as jnp
from jax import lax
from jax.experimental import pallas as pl
from jax.experimental.pallas import tpu as pltpu
from jax.sharding import Mesh
from jax.sharding import PartitionSpec as P

ROW_AXES = ("yh", "z2", "z1", "z0")
COLUMN_AXES = ("y1", "y0", "x1", "x0", "co")
ORDER = ("y1", "y0", "x0", "z1", "z0", "yh", "z2")
BACK_ORDER = ("y1", "y0", "z1", "z0", "yh", "z2")
EPS = 1e-05
F32 = jnp.float32
BF16 = jnp.bfloat16


def lane_iota(shape):
    return lax.broadcasted_iota(jnp.int32, shape, len(shape) - 1)


def swap_bits(arrays, bits):
    arrays = list(arrays)
    lanes = lane_iota(arrays[0].shape)
    for pos, lane in bits:
        step, width = 1 << pos, 1 << lane
        high = (lanes & width) != 0
        for at in range(len(arrays)):
            if at & step:
                continue
            a, b = arrays[at], arrays[at + step]
            arrays[at] = jnp.where(high, pltpu.roll(b, width, 1), a)
            arrays[at + step] = jnp.where(high, b, pltpu.roll(a, 128 - width, 1))
    return arrays


def project_kernel(
    pair_hbm,
    weight_hbm,
    mask_hbm,
    gain_hbm,
    bias_hbm,
    out_gain_hbm,
    out_bias_hbm,
    sent,
    normed_out,
    scales,
    pair,
    weight,
    mask,
    gain,
    bias,
    rows,
    sems,
):
    moves = (
        (pair_hbm, pair),
        (gain_hbm, gain),
        (bias_hbm, bias),
        (weight_hbm, weight),
        (mask_hbm, mask),
        (out_gain_hbm, scales.at[pl.ds(0, 1)]),
        (out_bias_hbm, scales.at[pl.ds(1, 1)]),
    )
    copies = [
        pltpu.make_async_copy(source, target, sems.at[at])
        for at, (source, target) in enumerate(moves)
    ]
    for copy in copies:
        copy.start()
    copies[0].wait()
    x = pair[...].astype(F32)
    centered = x - jnp.mean(x, axis=-1, keepdims=True)
    variance = jnp.mean(centered * centered, axis=-1, keepdims=True)
    normalized = centered * lax.rsqrt(variance + EPS)
    for copy in copies[1:]:
        copy.wait()
    normed = (normalized * gain[...] + bias[...]).astype(BF16)
    normed_out[...] = normed
    k_of_lane = lane_iota((16, 128)) & 15
    spread = (k_of_lane == lax.broadcasted_iota(jnp.int32, (16, 128), 0)).astype(BF16)
    masks = lax.dot_general(
        mask[...].astype(F32).astype(BF16),
        spread,
        (((0,), (0,)), ((), ())),
        preferred_element_type=F32,
    )
    own_row = (lane_iota((8, 128)) >> 4) == lax.broadcasted_iota(jnp.int32, (8, 128), 0)
    for q in range(4):
        projected = lax.dot_general(
            weight[...],
            normed[q * 128 : (q + 1) * 128],
            (((0,), (1,)), ((), ())),
            preferred_element_type=F32,
        )
        keep = jnp.sum(jnp.where(own_row, masks[q * 8 : (q + 1) * 8], 0.0), axis=0, keepdims=True)
        rows[pl.ds(q * 2, 128, stride=8), :] = (
            jax.nn.sigmoid(projected[:128]) * projected[128:256] * keep
        )
        rows[pl.ds((q % 2 * 2 + q // 2) * 2 + 1, 128, stride=8), :] = (
            jax.nn.sigmoid(projected[256:384]) * projected[384:] * keep
        )
    sent[...] = rows[...].astype(BF16)


def residues_in_lanes(rows, start, size, stride):
    pieces = [rows[pl.ds(start + g * 128, size, stride=stride), :] for g in range(8)]
    return swap_bits(pieces, ((0, 4), (1, 5), (2, 6)))


def partial_kernel(got, sent, left, right, rows):
    rows[...] = got[...].astype(F32)
    for z in range(4):
        for r, piece in enumerate(residues_in_lanes(rows, z * 32, 16, 2)):
            left[pl.ds(z * 128 + r * 16, 16), :] = piece.astype(BF16)
        for core in range(2):
            pieces = residues_in_lanes(rows, z * 32 + core * 2 + 1, 8, 4)
            for r in range(0, 8, 2):
                both = jnp.concatenate(pieces[r : r + 2], axis=0)
                right[pl.ds(z * 128 + core * 64 + r * 8, 16), :] = both.astype(BF16)
    for z in range(4):
        block = pl.ds(z * 128, 128)
        sent[block, :] = lax.dot_general(
            right[block, :], left[...], (((1,), (1,)), ((), ())), preferred_element_type=F32
        ).astype(BF16)


def sum_kernel(got, sent, total, rows):
    for x0 in range(2):
        for z in range(4):
            base = (x0 * 4 + z) * 64
            total[pl.ds(base, 64), :] = sum(
                got[pl.ds((x1 * 4 + x0 * 2 + core) * 64, 64), pl.ds(z * 128, 128)].astype(F32)
                for x1 in range(2)
                for core in range(2)
            )
            for jh in range(2):
                pieces = [total[pl.ds(base + t * 16 + jh, 8, stride=2), :] for t in range(4)]
                pieces = swap_bits(pieces, ((0, 2), (1, 3)))
                for v in range(4):
                    for low in range(2):
                        at = (z * 4 + v) * 8 + x0 * 4 + jh * 2 + low
                        rows[pl.ds(at, 4, stride=128), :] = pieces[v][low * 4 : low * 4 + 4]
    sent[...] = rows[0:512, :].astype(BF16)


def mix_kernel(
    got, normed, gate_weight, scales, out_weight, update, rows, mixed, ordered, staged, sems
):
    rows[...] = got[...].astype(F32)
    gains = jnp.broadcast_to(scales[0:1, :], (128, 128)).T
    biases = jnp.broadcast_to(scales[1:2, :], (128, 128)).T
    for h in range(4):
        triangle = jnp.concatenate(
            [
                rows[pl.ds(y * 128 + x0 * 4 + h, 16, stride=8), :]
                for y in range(4)
                for x0 in range(2)
            ],
            axis=0,
        )
        centered = triangle - jnp.mean(triangle, axis=0, keepdims=True)
        variance = jnp.mean(centered * centered, axis=0, keepdims=True)
        tri_normed = (centered * lax.rsqrt(variance + EPS) * gains + biases).astype(BF16)
        mixed[pl.ds(h * 128, 128), :] = lax.dot_general(
            tri_normed, out_weight[...], (((0,), (0,)), ((), ())), preferred_element_type=F32
        )
    copies = []
    for s in range(4):
        block = pl.ds(s * 128, 128)
        gating = jax.nn.sigmoid(
            jnp.dot(normed[block, :], gate_weight[...], preferred_element_type=F32)
        )
        for h in range(4):
            for jj in range(4):
                column = h // 2 * 8 + jj * 2 + h % 2
                ordered[pl.ds(s * 128 + column, 8, stride=16), :] = mixed[
                    pl.ds(h * 128 + jj * 4 + s, 8, stride=16), :
                ]
        staged[block, :] = (ordered[block, :] * gating).astype(BF16)
        copies.append(pltpu.make_async_copy(staged.at[block], update.at[block], sems.at[s]))
        copies[s].start()
    for copy in copies:
        copy.wait()


def local_call(kernel, outs, scratch=(), in_space=pltpu.VMEM, out_space=pltpu.VMEM):

    def call(*args):
        return pl.pallas_call(
            kernel,
            out_shape=outs,
            in_specs=[pl.BlockSpec(memory_space=in_space)] * len(args),
            out_specs=jax.tree.map(lambda _: pl.BlockSpec(memory_space=out_space), outs),
            scratch_shapes=scratch,
            compiler_params=pltpu.CompilerParams(vmem_limit_bytes=16 << 20),
            cost_estimate=pl.CostEstimate(
                flops=1_000_000, bytes_accessed=1 << 20, transcendentals=0
            ),
        )(*args)

    return call


def on_device(
    pair, pair_mask, in_gain, in_bias, proj_weight, gate_weight, out_gain, out_bias, out_weight
):
    shape = jax.ShapeDtypeStruct
    inputs = (
        pair.reshape(512, 128),
        proj_weight,
        pair_mask.T,
        in_gain[None],
        in_bias[None],
        out_gain[None],
        out_bias[None],
    )
    sent, normed, scales = local_call(
        project_kernel,
        (shape((1024, 128), BF16), shape((512, 128), BF16), shape((2, 128), F32)),
        [
            pltpu.VMEM((512, 128), BF16),
            pltpu.VMEM((128, 512), BF16),
            pltpu.VMEM((16, 32), jnp.int32),
            pltpu.VMEM((1, 128), F32),
            pltpu.VMEM((1, 128), F32),
            pltpu.VMEM((1024, 128), F32),
            pltpu.SemaphoreType.DMA((7,)),
        ],
        in_space=pltpu.HBM,
    )(*(pltpu.with_memory_space_constraint(a, pltpu.HBM) for a in inputs))
    got = lax.all_to_all(sent.reshape(128, 8, 128), ORDER, 0, 0, tiled=True)
    side = pltpu.VMEM((512, 128), BF16)
    partial = local_call(
        partial_kernel, shape((512, 512), BF16), [side, side, pltpu.VMEM((1024, 128), F32)]
    )(got.reshape(1024, 128))
    parts = lax.all_to_all(partial.reshape(8, 64, 512), ("x1", "x0", "co"), 0, 0, tiled=True)
    sums = local_call(
        sum_kernel,
        shape((512, 128), BF16),
        [pltpu.VMEM((512, 128), F32), pltpu.VMEM((1024, 128), F32)],
    )(parts.reshape(512, 512))
    back = lax.all_to_all(sums.reshape(64, 8, 128), BACK_ORDER, 0, 0, tiled=True)
    block = pltpu.VMEM((512, 128), F32)
    update = local_call(
        mix_kernel,
        shape((512, 128), BF16),
        [block, block, block, pltpu.VMEM((512, 128), BF16), pltpu.SemaphoreType.DMA((4,))],
        out_space=pltpu.HBM,
    )(back.reshape(512, 128), normed, gate_weight, scales, out_weight)
    return update.reshape(32, 16, 128)


def solution(mesh):
    finer = Mesh(mesh.devices.reshape((2,) * 9), ROW_AXES + COLUMN_AXES)
    in_specs = (
        P(ROW_AXES, COLUMN_AXES, None),
        P(ROW_AXES, COLUMN_AXES),
        P(),
        P(),
        P(),
        P(),
        P(),
        P(),
        P(),
    )
    return jax.shard_map(
        on_device,
        mesh=finer,
        in_specs=in_specs,
        out_specs=P(ROW_AXES, COLUMN_AXES, None),
        check_vma=False,
    )
```

```python
import jax
import jax.numpy as jnp
from jax import lax
from jax.experimental import pallas as pl
from jax.experimental.pallas import tpu as pltpu
from jax.sharding import Mesh
from jax.sharding import PartitionSpec as P

ROW_AXES = ("yh", "z2", "z1", "z0")
COLUMN_AXES = ("y1", "y0", "x1", "x0", "co")
ORDER = ("y0", "y1", "co", "z1", "z0", "z2", "yh")
BACK_ORDER = ("y0", "y1", "z1", "z0", "z2", "yh")
EPS = 1e-05
F32 = jnp.float32
BF16 = jnp.bfloat16


def lane_iota(shape):
    return lax.broadcasted_iota(jnp.int32, shape, len(shape) - 1)


def swap_bits(arrays, bits):
    arrays = list(arrays)
    lanes = lane_iota(arrays[0].shape)
    for pos, lane in bits:
        step, width = 1 << pos, 1 << lane
        high = (lanes & width) != 0
        for at in range(len(arrays)):
            if at & step:
                continue
            a, b = arrays[at], arrays[at + step]
            arrays[at] = jnp.where(high, pltpu.roll(b, width, 1), a)
            arrays[at + step] = jnp.where(high, b, pltpu.roll(a, 128 - width, 1))
    return arrays


def project_kernel(
    pair_hbm,
    weight_hbm,
    mask_hbm,
    gain_hbm,
    bias_hbm,
    out_gain_hbm,
    out_bias_hbm,
    sent,
    normed_out,
    scales,
    pair,
    weight,
    mask,
    gain,
    bias,
    rows,
    sems,
):
    moves = (
        (pair_hbm, pair),
        (gain_hbm, gain),
        (bias_hbm, bias),
        (weight_hbm, weight),
        (mask_hbm, mask),
        (out_gain_hbm, scales.at[pl.ds(0, 1)]),
        (out_bias_hbm, scales.at[pl.ds(1, 1)]),
    )
    copies = [
        pltpu.make_async_copy(source, target, sems.at[at])
        for at, (source, target) in enumerate(moves)
    ]
    for copy in copies:
        copy.start()
    copies[0].wait()
    x = pair[...].astype(F32)
    centered = x - jnp.mean(x, axis=-1, keepdims=True)
    variance = jnp.mean(centered * centered, axis=-1, keepdims=True)
    normalized = centered * lax.rsqrt(variance + EPS)
    for copy in copies[1:]:
        copy.wait()
    normed = (normalized * gain[...] + bias[...]).astype(BF16)
    normed_out[...] = normed
    k_of_lane = lane_iota((16, 128)) & 15
    spread = (k_of_lane == lax.broadcasted_iota(jnp.int32, (16, 128), 0)).astype(BF16)
    masks = lax.dot_general(
        mask[...].astype(F32).astype(BF16),
        spread,
        (((0,), (0,)), ((), ())),
        preferred_element_type=F32,
    )
    own_row = (lane_iota((8, 128)) >> 4) == lax.broadcasted_iota(jnp.int32, (8, 128), 0)
    for q in range(4):
        projected = lax.dot_general(
            weight[...],
            normed[q * 128 : (q + 1) * 128],
            (((0,), (1,)), ((), ())),
            preferred_element_type=F32,
        )
        keep = jnp.sum(jnp.where(own_row, masks[q * 8 : (q + 1) * 8], 0.0), axis=0, keepdims=True)
        rows[pl.ds(q * 2, 128, stride=8), :] = (
            jax.nn.sigmoid(projected[:128]) * projected[128:256] * keep
        )
        rows[pl.ds((q % 2 * 2 + q // 2) * 2 + 1, 128, stride=8), :] = (
            jax.nn.sigmoid(projected[256:384]) * projected[384:] * keep
        )
    sent[...] = rows[...].astype(BF16)


def residues_in_lanes(rows, start, size, stride):
    pieces = [rows[pl.ds(start + g * 128, size, stride=stride), :] for g in range(8)]
    return swap_bits(pieces, ((0, 4), (1, 5), (2, 6)))


def partial_kernel(got, sent, left, right, rows):
    rows[...] = got[...].astype(F32)
    for z in range(4):
        for r, piece in enumerate(residues_in_lanes(rows, z * 32, 16, 2)):
            left[pl.ds(z * 128 + r * 16, 16), :] = piece.astype(BF16)
        for core in range(2):
            pieces = residues_in_lanes(rows, z * 32 + core * 2 + 1, 8, 4)
            for r in range(0, 8, 2):
                both = jnp.concatenate(pieces[r : r + 2], axis=0)
                right[pl.ds(z * 128 + core * 64 + r * 8, 16), :] = both.astype(BF16)
    for z in range(4):
        block = pl.ds(z * 128, 128)
        sent[block, :] = lax.dot_general(
            right[block, :], left[...], (((1,), (1,)), ((), ())), preferred_element_type=F32
        ).astype(BF16)


def sum_kernel(got, sent, total, rows):
    for core in range(2):
        for z in range(4):
            base = (core * 4 + z) * 64
            total[pl.ds(base, 64), :] = sum(
                got[pl.ds((x * 2 + core) * 64, 64), pl.ds(z * 128, 128)].astype(F32)
                for x in range(4)
            )
            for jh in range(2):
                pieces = [total[pl.ds(base + t * 16 + jh, 8, stride=2), :] for t in range(4)]
                pieces = swap_bits(pieces, ((0, 2), (1, 3)))
                for v in range(4):
                    for low in range(2):
                        at = (z * 4 + v) * 8 + core * 4 + jh * 2 + low
                        rows[pl.ds(at, 4, stride=128), :] = pieces[v][low * 4 : low * 4 + 4]
    sent[...] = rows[0:512, :].astype(BF16)


def mix_kernel(
    got, normed, gate_weight, scales, out_weight, update, rows, mixed, ordered, staged, sems
):
    rows[...] = got[...].astype(F32)
    gains = jnp.broadcast_to(scales[0:1, :], (128, 128)).T
    biases = jnp.broadcast_to(scales[1:2, :], (128, 128)).T
    for h in range(4):
        triangle = jnp.concatenate(
            [
                rows[pl.ds(y * 128 + core * 4 + h, 16, stride=8), :]
                for y in range(4)
                for core in range(2)
            ],
            axis=0,
        )
        centered = triangle - jnp.mean(triangle, axis=0, keepdims=True)
        variance = jnp.mean(centered * centered, axis=0, keepdims=True)
        tri_normed = (centered * lax.rsqrt(variance + EPS) * gains + biases).astype(BF16)
        mixed[pl.ds(h * 128, 128), :] = lax.dot_general(
            tri_normed, out_weight[...], (((0,), (0,)), ((), ())), preferred_element_type=F32
        )
    copies = []
    for s in range(4):
        block = pl.ds(s * 128, 128)
        gating = jax.nn.sigmoid(
            jnp.dot(normed[block, :], gate_weight[...], preferred_element_type=F32)
        )
        for h in range(4):
            for jj in range(4):
                column = h // 2 * 8 + jj * 2 + h % 2
                ordered[pl.ds(s * 128 + column, 8, stride=16), :] = mixed[
                    pl.ds(h * 128 + jj * 4 + s, 8, stride=16), :
                ]
        staged[block, :] = (ordered[block, :] * gating).astype(BF16)
        copies.append(pltpu.make_async_copy(staged.at[block], update.at[block], sems.at[s]))
        copies[s].start()
    for copy in copies:
        copy.wait()


def local_call(kernel, outs, scratch=(), in_space=pltpu.VMEM, out_space=pltpu.VMEM):

    def call(*args):
        return pl.pallas_call(
            kernel,
            out_shape=outs,
            in_specs=[pl.BlockSpec(memory_space=in_space)] * len(args),
            out_specs=jax.tree.map(lambda _: pl.BlockSpec(memory_space=out_space), outs),
            scratch_shapes=scratch,
            compiler_params=pltpu.CompilerParams(vmem_limit_bytes=16 << 20),
            cost_estimate=pl.CostEstimate(
                flops=1_000_000, bytes_accessed=1 << 20, transcendentals=0
            ),
        )(*args)

    return call


def on_device(
    pair, pair_mask, in_gain, in_bias, proj_weight, gate_weight, out_gain, out_bias, out_weight
):
    shape = jax.ShapeDtypeStruct
    inputs = (
        pair.reshape(512, 128),
        proj_weight,
        pair_mask.T,
        in_gain[None],
        in_bias[None],
        out_gain[None],
        out_bias[None],
    )
    sent, normed, scales = local_call(
        project_kernel,
        (shape((1024, 128), BF16), shape((512, 128), BF16), shape((2, 128), F32)),
        [
            pltpu.VMEM((512, 128), BF16),
            pltpu.VMEM((128, 512), BF16),
            pltpu.VMEM((16, 32), jnp.int32),
            pltpu.VMEM((1, 128), F32),
            pltpu.VMEM((1, 128), F32),
            pltpu.VMEM((1024, 128), F32),
            pltpu.SemaphoreType.DMA((7,)),
        ],
        in_space=pltpu.HBM,
    )(*(pltpu.with_memory_space_constraint(a, pltpu.HBM) for a in inputs))
    got = lax.all_to_all(sent.reshape(128, 8, 128), ORDER, 0, 0, tiled=True)
    side = pltpu.VMEM((512, 128), BF16)
    partial = local_call(
        partial_kernel, shape((512, 512), BF16), [side, side, pltpu.VMEM((1024, 128), F32)]
    )(got.reshape(1024, 128))
    parts = lax.all_to_all(partial.reshape(8, 64, 512), ("x1", "x0", "co"), 0, 0, tiled=True)
    sums = local_call(
        sum_kernel,
        shape((512, 128), BF16),
        [pltpu.VMEM((512, 128), F32), pltpu.VMEM((1024, 128), F32)],
    )(parts.reshape(512, 512))
    back = lax.all_to_all(sums.reshape(64, 8, 128), BACK_ORDER, 0, 0, tiled=True)
    block = pltpu.VMEM((512, 128), F32)
    update = local_call(
        mix_kernel,
        shape((512, 128), BF16),
        [block, block, block, pltpu.VMEM((512, 128), BF16), pltpu.SemaphoreType.DMA((4,))],
        out_space=pltpu.HBM,
    )(back.reshape(512, 128), normed, gate_weight, scales, out_weight)
    return update.reshape(32, 16, 128)


def solution(mesh):
    finer = Mesh(mesh.devices.reshape((2,) * 9), ROW_AXES + COLUMN_AXES)
    in_specs = (
        P(ROW_AXES, COLUMN_AXES, None),
        P(ROW_AXES, COLUMN_AXES),
        P(),
        P(),
        P(),
        P(),
        P(),
        P(),
        P(),
    )
    return jax.shard_map(
        on_device,
        mesh=finer,
        in_specs=in_specs,
        out_specs=P(ROW_AXES, COLUMN_AXES, None),
        check_vma=False,
    )
```

```python
import jax
import jax.numpy as jnp
from jax import lax
from jax.experimental import pallas as pl
from jax.experimental.pallas import tpu as pltpu
from jax.sharding import Mesh
from jax.sharding import PartitionSpec as P

ROW_AXES = ("yh", "z2", "z1", "z0")
COLUMN_AXES = ("y1", "y0", "x1", "x0", "co")
ORDER = ("y1", "y0", "co", "z1", "z0", "yh", "z2")
BACK_ORDER = ("y1", "y0", "z1", "z0", "yh", "z2")
EPS = 1e-05
F32 = jnp.float32
BF16 = jnp.bfloat16


def lane_iota(shape):
    return lax.broadcasted_iota(jnp.int32, shape, len(shape) - 1)


def swap_bits(arrays, bits):
    arrays = list(arrays)
    lanes = lane_iota(arrays[0].shape)
    for pos, lane in bits:
        step, width = 1 << pos, 1 << lane
        high = (lanes & width) != 0
        for at in range(len(arrays)):
            if at & step:
                continue
            a, b = arrays[at], arrays[at + step]
            arrays[at] = jnp.where(high, pltpu.roll(b, width, 1), a)
            arrays[at + step] = jnp.where(high, b, pltpu.roll(a, 128 - width, 1))
    return arrays


def project_kernel(
    pair_hbm,
    weight_hbm,
    mask_hbm,
    gain_hbm,
    bias_hbm,
    out_gain_hbm,
    out_bias_hbm,
    sent,
    normed_out,
    scales,
    pair,
    weight,
    mask,
    gain,
    bias,
    rows,
    sems,
):
    moves = (
        (pair_hbm, pair),
        (gain_hbm, gain),
        (bias_hbm, bias),
        (weight_hbm, weight),
        (mask_hbm, mask),
        (out_gain_hbm, scales.at[pl.ds(0, 1)]),
        (out_bias_hbm, scales.at[pl.ds(1, 1)]),
    )
    copies = [
        pltpu.make_async_copy(source, target, sems.at[at])
        for at, (source, target) in enumerate(moves)
    ]
    for copy in copies:
        copy.start()
    copies[0].wait()
    x = pair[...].astype(F32)
    centered = x - jnp.mean(x, axis=-1, keepdims=True)
    variance = jnp.mean(centered * centered, axis=-1, keepdims=True)
    normalized = centered * lax.rsqrt(variance + EPS)
    for copy in copies[1:]:
        copy.wait()
    normed = (normalized * gain[...] + bias[...]).astype(BF16)
    normed_out[...] = normed
    k_of_lane = lane_iota((16, 128)) & 15
    spread = (k_of_lane == lax.broadcasted_iota(jnp.int32, (16, 128), 0)).astype(BF16)
    masks = lax.dot_general(
        mask[...].astype(F32).astype(BF16),
        spread,
        (((0,), (0,)), ((), ())),
        preferred_element_type=F32,
    )
    own_row = (lane_iota((8, 128)) >> 4) == lax.broadcasted_iota(jnp.int32, (8, 128), 0)
    for q in range(4):
        projected = lax.dot_general(
            weight[...],
            normed[q * 128 : (q + 1) * 128],
            (((0,), (1,)), ((), ())),
            preferred_element_type=F32,
        )
        keep = jnp.sum(jnp.where(own_row, masks[q * 8 : (q + 1) * 8], 0.0), axis=0, keepdims=True)
        rows[pl.ds(q * 2, 128, stride=8), :] = (
            jax.nn.sigmoid(projected[:128]) * projected[128:256] * keep
        )
        rows[pl.ds((q % 2 * 2 + q // 2) * 2 + 1, 128, stride=8), :] = (
            jax.nn.sigmoid(projected[256:384]) * projected[384:] * keep
        )
    sent[...] = rows[...].astype(BF16)


def residues_in_lanes(rows, start, size, stride):
    pieces = [rows[pl.ds(start + g * 128, size, stride=stride), :] for g in range(8)]
    return swap_bits(pieces, ((0, 4), (1, 5), (2, 6)))


def partial_kernel(got, sent, left, rows):
    rows[...] = got[...].astype(F32)
    for z in range(4):
        for r, piece in enumerate(residues_in_lanes(rows, z * 32, 16, 2)):
            left[pl.ds(z * 128 + r * 16, 16), :] = piece.astype(BF16)
    for z in range(4):
        pieces = [
            *residues_in_lanes(rows, z * 32 + 1, 8, 4),
            *residues_in_lanes(rows, z * 32 + 3, 8, 4),
        ]
        right = jnp.concatenate(pieces, axis=0).astype(BF16)
        sent[pl.ds(z * 128, 128), :] = lax.dot_general(
            right, left[...], (((1,), (1,)), ((), ())), preferred_element_type=F32
        ).astype(BF16)


def sum_kernel(got, sent, total, rows):
    for core in range(2):
        for z in range(4):
            base = (core * 4 + z) * 64
            total[pl.ds(base, 64), :] = sum(
                got[pl.ds((x * 2 + core) * 64, 64), pl.ds(z * 128, 128)].astype(F32)
                for x in range(4)
            )
            for jh in range(2):
                pieces = [total[pl.ds(base + t * 16 + jh, 8, stride=2), :] for t in range(4)]
                pieces = swap_bits(pieces, ((0, 2), (1, 3)))
                for v in range(4):
                    for low in range(2):
                        at = (z * 4 + v) * 8 + core * 4 + jh * 2 + low
                        rows[pl.ds(at, 4, stride=128), :] = pieces[v][low * 4 : low * 4 + 4]
    sent[...] = rows[0:512, :].astype(BF16)


def mix_kernel(
    got, normed, gate_weight, scales, out_weight, update, rows, mixed, ordered, staged, sems
):
    rows[...] = got[...].astype(F32)
    gains = jnp.broadcast_to(scales[0:1, :], (128, 128)).T
    biases = jnp.broadcast_to(scales[1:2, :], (128, 128)).T
    for h in range(4):
        triangle = jnp.concatenate(
            [
                rows[pl.ds(y * 128 + core * 4 + h, 16, stride=8), :]
                for y in range(4)
                for core in range(2)
            ],
            axis=0,
        )
        centered = triangle - jnp.mean(triangle, axis=0, keepdims=True)
        variance = jnp.mean(centered * centered, axis=0, keepdims=True)
        tri_normed = (centered * lax.rsqrt(variance + EPS) * gains + biases).astype(BF16)
        mixed[pl.ds(h * 128, 128), :] = lax.dot_general(
            tri_normed, out_weight[...], (((0,), (0,)), ((), ())), preferred_element_type=F32
        )
    copies = []
    for s in range(4):
        block = pl.ds(s * 128, 128)
        gating = jax.nn.sigmoid(
            jnp.dot(normed[block, :], gate_weight[...], preferred_element_type=F32)
        )
        for h in range(4):
            for jj in range(4):
                column = h // 2 * 8 + jj * 2 + h % 2
                ordered[pl.ds(s * 128 + column, 8, stride=16), :] = mixed[
                    pl.ds(h * 128 + jj * 4 + s, 8, stride=16), :
                ]
        staged[block, :] = (ordered[block, :] * gating).astype(BF16)
        copies.append(pltpu.make_async_copy(staged.at[block], update.at[block], sems.at[s]))
        copies[s].start()
    for copy in copies:
        copy.wait()


def local_call(kernel, outs, scratch=(), in_space=pltpu.VMEM, out_space=pltpu.VMEM):

    def call(*args):
        return pl.pallas_call(
            kernel,
            out_shape=outs,
            in_specs=[pl.BlockSpec(memory_space=in_space)] * len(args),
            out_specs=jax.tree.map(lambda _: pl.BlockSpec(memory_space=out_space), outs),
            scratch_shapes=scratch,
            compiler_params=pltpu.CompilerParams(vmem_limit_bytes=16 << 20),
            cost_estimate=pl.CostEstimate(
                flops=1_000_000, bytes_accessed=1 << 20, transcendentals=0
            ),
        )(*args)

    return call


def on_device(
    pair, pair_mask, in_gain, in_bias, proj_weight, gate_weight, out_gain, out_bias, out_weight
):
    shape = jax.ShapeDtypeStruct
    inputs = (
        pair.reshape(512, 128),
        proj_weight,
        pair_mask.T,
        in_gain[None],
        in_bias[None],
        out_gain[None],
        out_bias[None],
    )
    sent, normed, scales = local_call(
        project_kernel,
        (shape((1024, 128), BF16), shape((512, 128), BF16), shape((2, 128), F32)),
        [
            pltpu.VMEM((512, 128), BF16),
            pltpu.VMEM((128, 512), BF16),
            pltpu.VMEM((16, 32), jnp.int32),
            pltpu.VMEM((1, 128), F32),
            pltpu.VMEM((1, 128), F32),
            pltpu.VMEM((1024, 128), F32),
            pltpu.SemaphoreType.DMA((7,)),
        ],
        in_space=pltpu.HBM,
    )(*(pltpu.with_memory_space_constraint(a, pltpu.HBM) for a in inputs))
    got = lax.all_to_all(sent.reshape(128, 8, 128), ORDER, 0, 0, tiled=True)
    side = pltpu.VMEM((512, 128), BF16)
    partial = local_call(
        partial_kernel, shape((512, 512), BF16), [side, pltpu.VMEM((1024, 128), F32)]
    )(got.reshape(1024, 128))
    parts = lax.all_to_all(partial.reshape(8, 64, 512), ("x1", "x0", "co"), 0, 0, tiled=True)
    sums = local_call(
        sum_kernel,
        shape((512, 128), BF16),
        [pltpu.VMEM((512, 128), F32), pltpu.VMEM((1024, 128), F32)],
    )(parts.reshape(512, 512))
    back = lax.all_to_all(sums.reshape(64, 8, 128), BACK_ORDER, 0, 0, tiled=True)
    block = pltpu.VMEM((512, 128), F32)
    update = local_call(
        mix_kernel,
        shape((512, 128), BF16),
        [block, block, block, pltpu.VMEM((512, 128), BF16), pltpu.SemaphoreType.DMA((4,))],
        out_space=pltpu.HBM,
    )(back.reshape(512, 128), normed, gate_weight, scales, out_weight)
    return update.reshape(32, 16, 128)


def solution(mesh):
    finer = Mesh(mesh.devices.reshape((2,) * 9), ROW_AXES + COLUMN_AXES)
    in_specs = (
        P(ROW_AXES, COLUMN_AXES, None),
        P(ROW_AXES, COLUMN_AXES),
        P(),
        P(),
        P(),
        P(),
        P(),
        P(),
        P(),
    )
    return jax.shard_map(
        on_device,
        mesh=finer,
        in_specs=in_specs,
        out_specs=P(ROW_AXES, COLUMN_AXES, None),
        check_vma=False,
    )
```
